64 devices in a mesh: data: 4 (over x, y), tp: 16 (over z, core).
Axes of the slice: x: 2, y: 2, z: 8, core: 2. Of those that a mesh axis runs over, the one named last changes fastest.
The devices are a block of a 4x4x8 slice.
Arguments:
- x: bfloat16 [1024, 49152], P('data', 'tp'), parts along dimension 0
- w: bfloat16 [49152, 12288], P('tp')
- lengths: int32 [16], P('data'), parts along dimension 0
Outputs:
- output: bfloat16 [1024, 12288], P('data'), parts along dimension 0
There are 4 independent parts. The reference program is written for one: setup_inputs(seed, part) draws one part's arguments, and reference() takes and returns one part's arrays. A program takes and returns all parts, laid end to end along the dimension named above; an argument that names none is the same for every part.
All inputs are finite; a program needn't handle non-finite values.
Results may differ from the reference program's by a relative error of at most 0.001.
Values are sent between devices in bfloat16 or wider.
A program may use at most 768 MiB of HBM per device.

```python
import jax
import jax.numpy as jnp

D = 12288
FF = 49152
TOKENS = 256
SEQS = 4
SEQ_LEN = TOKENS // SEQS


def draw_lengths(key_len):
    key_draw, key_perm = jax.random.split(key_len)
    lengths = jax.random.randint(key_draw, (SEQS,), 1, SEQ_LEN + 1, dtype=jnp.int32)
    slot_order = jax.random.permutation(key_perm, SEQS)
    lengths = lengths.at[slot_order[0]].set(SEQ_LEN)
    lengths = lengths.at[slot_order[1]].set(1)
    return lengths


def setup_inputs(seed: int = 0, part: int = 0) -> dict:
    key = jax.random.key(seed)
    key_x, key_w, key_len = jax.random.split(key, 3)
    tok_acts = jax.random.normal(jax.random.fold_in(key_x, part), (TOKENS, FF), jnp.float32)
    weight = jax.random.normal(key_w, (FF, D), jnp.float32) * (FF ** -0.5)
    lengths = draw_lengths(jax.random.fold_in(key_len, part))
    return {"x": tok_acts.astype(jnp.bfloat16), "w": weight.astype(jnp.bfloat16), "lengths": lengths}


def reference(x, w, lengths):
    seq_len = x.shape[0] // lengths.shape[0]
    valid = (jnp.arange(seq_len, dtype=jnp.int32)[None, :] < lengths[:, None]).reshape(-1)
    full_sum = jnp.dot(x, w, preferred_element_type=jnp.float32)
    return jnp.where(valid[:, None], full_sum, 0.0).astype(jnp.bfloat16)
```

```python
import functools

import jax
import jax.numpy as jnp
from jax import lax
from jax.experimental import pallas as pl
from jax.experimental.pallas import tpu as pltpu
from jax.sharding import PartitionSpec as P

MESH = pl.DeviceIdType.MESH
LANES = 128
CORES = 2
DIRS = 2
UNITS = 3
LAG = 3


def first_single(len_ref, n_seq):
    slot = jnp.int32(n_seq - 1)
    for s in reversed(range(n_seq - 1)):
        slot = jnp.where(len_ref[s] == 1, jnp.int32(s), slot)
    return slot


def reduce_kernel(
    chips, n_seq, seq_len,
    len_ref, x_hbm, w_hbm, y_hbm,
    x_raw, xc, wbuf, part, part_in, rs_in, ag, ag_pair,
    x_sem, w_sem, pp_send, pp_recv, rs_send, rs_recv, ag_send, ag_recv, ap_send, ap_recv, out_sem, outp_sem,
):
    me = lax.axis_index("tp")
    z, core = me // CORES, lax.rem(me, CORES)
    nxt = lax.rem(z + 1, chips) * CORES + core
    prv = lax.rem(z + chips - 1, chips) * CORES + core
    mate = z * CORES + (1 - core)
    towards = (nxt, prv)
    body_rows = (n_seq - 1) * seq_len
    lastc = chips - 1
    n_k = DIRS * UNITS

    def chunk_of(s, d):
        if d == 0:
            return lax.rem(z + (2 * chips - 1) - s, chips)
        return lax.rem(z + 1 + s, chips)

    def slot_chunk(h, d):
        if d == 0:
            return lax.rem(z + chips - h, chips)
        return lax.rem(z + h, chips)

    def w_copy(s, k):
        d, u = k % DIRS, k // DIRS
        col = ((chunk_of(s, d) * DIRS + d) * UNITS + u) * (CORES * LANES)
        col = pl.multiple_of(col, CORES * LANES)
        return pltpu.make_async_copy(w_hbm.at[:, pl.ds(col, CORES * LANES)], wbuf.at[k], w_sem.at[k])

    def f_rows(u):
        return pl.ds(u * body_rows, body_rows + (8 if u == UNITS - 1 else 0))

    def h_rows(u):
        return pl.ds(u * body_rows, body_rows + (16 if u == UNITS - 1 else 0))

    x_copy = pltpu.make_async_copy(x_hbm, x_raw, x_sem)
    x_copy.start()
    for k in range(n_k):
        w_copy(0, k).start()

    barrier = pltpu.get_barrier_semaphore()
    for peer in (mate, nxt, prv):
        pl.semaphore_signal(barrier, inc=1, device_id={"tp": peer}, device_id_type=MESH)

    single = first_single(len_ref, n_seq)
    x_copy.wait()
    def x_rows(slot, count):
        return x_raw[slot * seq_len:slot * seq_len + count, :]

    for p in range(n_seq - 1):
        xc[p * seq_len:(p + 1) * seq_len, :] = jnp.where(single <= p, x_rows(p + 1, seq_len), x_rows(p, seq_len))
    lone = x_rows(n_seq - 1, 16)
    for s in range(n_seq - 1):
        lone = jnp.where(single == s, x_rows(s, 16), lone)
    xc[body_rows:body_rows + 16, :] = lone
    pl.semaphore_wait(barrier, 3)

    def pp_copy(s, k):
        d, u = k % DIRS, k // DIRS
        return pltpu.make_async_remote_copy(
            src_ref=part.at[1 - core, s, d, f_rows(u)], dst_ref=part_in.at[s, d, f_rows(u)],
            send_sem=pp_send.at[s, k], recv_sem=pp_recv.at[s, k], device_id={"tp": mate}, device_id_type=MESH)

    def rs_copy(s, k):
        d, u = k % DIRS, k // DIRS
        return pltpu.make_async_remote_copy(
            src_ref=part.at[core, s, d, f_rows(u)], dst_ref=rs_in.at[s, d, f_rows(u)],
            send_sem=rs_send.at[s, k], recv_sem=rs_recv.at[s, k], device_id={"tp": towards[d]}, device_id_type=MESH)

    def ag_copy(h, k):
        d, u = k % DIRS, k // DIRS
        return pltpu.make_async_remote_copy(
            src_ref=ag.at[h, d, h_rows(u)], dst_ref=ag.at[h + 1, d, h_rows(u)],
            send_sem=ag_send.at[h, k], recv_sem=ag_recv.at[h, k], device_id={"tp": towards[d]}, device_id_type=MESH)

    def ap_copy(h, k):
        d, u = k % DIRS, k // DIRS
        return pltpu.make_async_remote_copy(
            src_ref=ag.at[h, d, h_rows(u)], dst_ref=ag_pair.at[h, d, h_rows(u)],
            send_sem=ap_send.at[h, k], recv_sem=ap_recv.at[h, k], device_id={"tp": mate}, device_id_type=MESH)

    def out_copy(h, k):
        d, u = k % DIRS, k // DIRS
        return pltpu.make_async_copy(
            ag.at[h, d, h_rows(u)], y_hbm.at[core, slot_chunk(h, d), d, h_rows(u)], out_sem.at[h, k])

    def outp_copy(h, k):
        d, u = k % DIRS, k // DIRS
        return pltpu.make_async_copy(
            ag_pair.at[h, d, h_rows(u)], y_hbm.at[1 - core, slot_chunk(h, d), d, h_rows(u)], outp_sem.at[h, k])

    def compute(s, k):
        d, u = k % DIRS, k // DIRS
        w_copy(s, k).wait()
        prod = jnp.dot(xc[...], wbuf[k], preferred_element_type=jnp.float32)
        for half in range(CORES):
            cols = slice(half * LANES, (half + 1) * LANES)
            part[half, s, d, u * body_rows:(u + 1) * body_rows, :] = prod[:body_rows, cols]
            tile = UNITS * body_rows
            if u == 0:
                part[half, s, d, tile:tile + 8, :] = prod[body_rows:body_rows + 8, cols]
            else:
                part[half, s, d, tile + u:tile + u + 1, :] = prod[body_rows:body_rows + 1, cols]
        pp_copy(s, k).start()

        @pl.when(s < lastc)
        def _():
            w_copy(s + 1, k).start()

    def ring(s, k):
        d, u = k % DIRS, k // DIRS
        rows = f_rows(u)
        pp_copy(s, k).wait_recv()

        @pl.when(s == 0)
        def _():
            part[core, s, d, rows, :] = part[core, s, d, rows, :] + part_in[s, d, rows, :]
            rs_copy(s, k).start()

        @pl.when(jnp.logical_and(s > 0, s < lastc))
        def _():
            rs_copy(s - 1, k).wait_recv()
            part[core, s, d, rows, :] = (part[core, s, d, rows, :] + part_in[s, d, rows, :]) + rs_in[s - 1, d, rows, :]
            rs_copy(s, k).start()

        @pl.when(s == lastc)
        def _():
            rs_copy(s - 1, k).wait_recv()
            total = (part[core, s, d, rows, :] + part_in[s, d, rows, :]) + rs_in[s - 1, d, rows, :]
            if u == UNITS - 1:
                total = jnp.concatenate([total, total[body_rows:, :]], axis=0)
            ag[0, d, h_rows(u), :] = total.astype(jnp.bfloat16)
            ag_copy(0, k).start()
            ap_copy(0, k).start()
            out_copy(0, k).start()

    @pl.loop(0, chips)
    def _(s):
        for k in range(n_k):
            compute(s, k)
            if k >= LAG:
                ring(s, k - LAG)
            else:
                @pl.when(s > 0)
                def _():
                    ring(s - 1, k + n_k - LAG)

    for k in range(n_k - LAG, n_k):
        ring(jnp.int32(lastc), k)

    @pl.loop(1, chips)
    def _(h):
        for k in range(n_k):
            ag_copy(h - 1, k).wait_recv()

            @pl.when(h < lastc)
            def _():
                ag_copy(h, k).start()

            ap_copy(h, k).start()
            out_copy(h, k).start()
            ap_copy(h - 1, k).wait_recv()
            outp_copy(h - 1, k).start()

    for k in range(n_k):
        ap_copy(lastc, k).wait_recv()
        outp_copy(lastc, k).start()

    @pl.loop(0, chips)
    def _(s):
        for k in range(n_k):
            pp_copy(s, k).wait_send()
            ap_copy(s, k).wait_send()
            out_copy(s, k).wait()
            outp_copy(s, k).wait()

            @pl.when(s < lastc)
            def _():
                rs_copy(s, k).wait_send()
                ag_copy(s, k).wait_send()


def expand_kernel(n_seq, seq_len, len_ref, y_ref, o_ref):
    body_rows = (n_seq - 1) * seq_len
    single = first_single(len_ref, n_seq)
    row = lax.broadcasted_iota(jnp.int32, (seq_len, LANES), 0)
    for u in range(UNITS):
        for core in range(CORES):
            cols = slice((u * CORES + core) * LANES, (u * CORES + core + 1) * LANES)
            tile = y_ref[core, 0, 0, UNITS * body_rows:UNITS * body_rows + 16, :].astype(jnp.float32)
            lone = jnp.broadcast_to(tile[u:u + 1, :], (seq_len, LANES))
            for s in range(n_seq):
                pos = jnp.minimum(s - (single < s).astype(jnp.int32), n_seq - 2)
                start = pl.multiple_of(u * body_rows + pos * seq_len, seq_len)
                rows = y_ref[core, 0, 0, pl.ds(start, seq_len), :].astype(jnp.float32)
                rows = jnp.where(single == s, lone, rows)
                o_ref[s * seq_len:(s + 1) * seq_len, cols] = jnp.where(row < len_ref[s], rows, 0.0).astype(o_ref.dtype)


def solution(mesh):
    chips = mesh.shape["tp"] // CORES

    def local_part(x_loc, w_loc, lengths):
        tokens, depth = x_loc.shape
        columns = w_loc.shape[1]
        n_seq = lengths.shape[0]
        seq_len = tokens // n_seq
        body_rows = (n_seq - 1) * seq_len
        n_k = DIRS * UNITS
        assert columns == chips * DIRS * UNITS * CORES * LANES
        f_tall, h_tall = UNITS * body_rows + 8, UNITS * body_rows + 16
        dma = pltpu.SemaphoreType.DMA
        packed = pl.pallas_call(
            functools.partial(reduce_kernel, chips, n_seq, seq_len),
            out_shape=jax.ShapeDtypeStruct((CORES, chips, DIRS, h_tall, LANES), jnp.bfloat16),
            in_specs=[
                pl.BlockSpec(memory_space=pltpu.SMEM),
                pl.BlockSpec(memory_space=pl.ANY),
                pl.BlockSpec(memory_space=pl.ANY),
            ],
            out_specs=pl.BlockSpec(memory_space=pl.ANY),
            scratch_shapes=[
                pltpu.VMEM((tokens, depth), jnp.bfloat16),
                pltpu.VMEM((body_rows + 16, depth), jnp.bfloat16),
                pltpu.VMEM((n_k, depth, CORES * LANES), jnp.bfloat16),
                pltpu.VMEM((CORES, chips, DIRS, f_tall, LANES), jnp.float32),
                pltpu.VMEM((chips, DIRS, f_tall, LANES), jnp.float32),
                pltpu.VMEM((chips - 1, DIRS, f_tall, LANES), jnp.float32),
                pltpu.VMEM((chips, DIRS, h_tall, LANES), jnp.bfloat16),
                pltpu.VMEM((chips, DIRS, h_tall, LANES), jnp.bfloat16),
                dma,
                dma((n_k,)),
                dma((chips, n_k)), dma((chips, n_k)),
                dma((chips - 1, n_k)), dma((chips - 1, n_k)),
                dma((chips - 1, n_k)), dma((chips - 1, n_k)),
                dma((chips, n_k)), dma((chips, n_k)),
                dma((chips, n_k)), dma((chips, n_k)),
            ],
            compiler_params=pltpu.CompilerParams(
                collective_id=0, has_side_effects=True, vmem_limit_bytes=60 * 1024 * 1024),
            name="reduce_gather",
        )(lengths, x_loc, w_loc)
        wide = UNITS * CORES * LANES
        return pl.pallas_call(
            functools.partial(expand_kernel, n_seq, seq_len),
            out_shape=jax.ShapeDtypeStruct((tokens, columns), jnp.bfloat16),
            grid=(chips * DIRS,),
            in_specs=[
                pl.BlockSpec(memory_space=pltpu.SMEM),
                pl.BlockSpec((CORES, 1, 1, h_tall, LANES), lambda i: (0, i // DIRS, i % DIRS, 0, 0)),
            ],
            out_specs=pl.BlockSpec((tokens, wide), lambda i: (0, i)),
            name="expand_rows",
        )(lengths, packed)

    return jax.shard_map(local_part, mesh=mesh, in_specs=(P("data", "tp"), P("tp", None), P("data")), out_specs=P("data", None), check_vma=False)
```

```python
import functools

import jax
import jax.numpy as jnp
from jax import lax
from jax.experimental import pallas as pl
from jax.experimental.pallas import tpu as pltpu
from jax.sharding import PartitionSpec as P

MESH = pl.DeviceIdType.MESH
LANES = 128
CORES = 2
DIRS = 2
UNITS = 3


def first_single(len_ref, n_seq):
    slot = jnp.int32(n_seq - 1)
    for s in reversed(range(n_seq - 1)):
        slot = jnp.where(len_ref[s] == 1, jnp.int32(s), slot)
    return slot


def reduce_kernel(
    chips, n_seq, seq_len,
    len_ref, x_hbm, w_hbm, ag, ag_pair,
    x_raw, xc, wbuf, part, part_in, rs_in,
    x_sem, w_sem, pp_send, pp_recv, rs_send, rs_recv, ag_send, ag_recv, ap_send, ap_recv,
):
    me = lax.axis_index("tp")
    z, core = me // CORES, lax.rem(me, CORES)
    nxt = lax.rem(z + 1, chips) * CORES + core
    prv = lax.rem(z + chips - 1, chips) * CORES + core
    mate = z * CORES + (1 - core)
    towards = (nxt, prv)
    body_rows = (n_seq - 1) * seq_len
    lastc = chips - 1
    n_k = DIRS * UNITS

    def chunk_of(s, d):
        if d == 0:
            return lax.rem(z + (2 * chips - 1) - s, chips)
        return lax.rem(z + 1 + s, chips)

    def w_copy(s, k):
        d, u = k % DIRS, k // DIRS
        col = ((chunk_of(s, d) * DIRS + d) * UNITS + u) * (CORES * LANES)
        col = pl.multiple_of(col, CORES * LANES)
        return pltpu.make_async_copy(w_hbm.at[:, pl.ds(col, CORES * LANES)], wbuf.at[u, :, pl.ds(d * CORES * LANES, CORES * LANES)], w_sem.at[k])

    def f_rows(u):
        return pl.ds(u * body_rows, body_rows + (8 if u == UNITS - 1 else 0))

    def h_rows(u):
        return pl.ds(u * body_rows, body_rows + (16 if u == UNITS - 1 else 0))

    x_copy = pltpu.make_async_copy(x_hbm, x_raw, x_sem)
    x_copy.start()
    for k in range(n_k):
        w_copy(0, k).start()

    barrier = pltpu.get_barrier_semaphore()
    for peer in (mate, nxt, prv):
        pl.semaphore_signal(barrier, inc=1, device_id={"tp": peer}, device_id_type=MESH)

    single = first_single(len_ref, n_seq)
    x_copy.wait()
    def x_rows(slot, count):
        return x_raw[slot * seq_len:slot * seq_len + count, :]

    for p in range(n_seq - 1):
        xc[p * seq_len:(p + 1) * seq_len, :] = jnp.where(single <= p, x_rows(p + 1, seq_len), x_rows(p, seq_len))
    lone = x_rows(n_seq - 1, 16)
    for s in range(n_seq - 1):
        lone = jnp.where(single == s, x_rows(s, 16), lone)
    xc[body_rows:body_rows + 16, :] = lone
    pl.semaphore_wait(barrier, 3)

    def pp_copy(s, k):
        d, u = k % DIRS, k // DIRS
        return pltpu.make_async_remote_copy(
            src_ref=part.at[1 - core, s, d, f_rows(u)], dst_ref=part_in.at[s, d, f_rows(u)],
            send_sem=pp_send.at[s, k], recv_sem=pp_recv.at[s, k], device_id={"tp": mate}, device_id_type=MESH)

    def rs_copy(s, k):
        d, u = k % DIRS, k // DIRS
        return pltpu.make_async_remote_copy(
            src_ref=part.at[core, s, d, f_rows(u)], dst_ref=rs_in.at[s, d, f_rows(u)],
            send_sem=rs_send.at[s, k], recv_sem=rs_recv.at[s, k], device_id={"tp": towards[d]}, device_id_type=MESH)

    def ag_copy(h, k):
        d, u = k % DIRS, k // DIRS
        return pltpu.make_async_remote_copy(
            src_ref=ag.at[h, d, h_rows(u)], dst_ref=ag.at[h + 1, d, h_rows(u)],
            send_sem=ag_send.at[h, k], recv_sem=ag_recv.at[h, k], device_id={"tp": towards[d]}, device_id_type=MESH)

    def ap_copy(h, k):
        d, u = k % DIRS, k // DIRS
        return pltpu.make_async_remote_copy(
            src_ref=ag.at[h, d, h_rows(u)], dst_ref=ag_pair.at[h, d, h_rows(u)],
            send_sem=ap_send.at[h, k], recv_sem=ap_recv.at[h, k], device_id={"tp": mate}, device_id_type=MESH)

    def compute(s, u):
        for d in range(DIRS):
            w_copy(s, u * DIRS + d).wait()
        prod = jnp.dot(xc[...], wbuf[u], preferred_element_type=jnp.float32)
        for d in range(DIRS):
            for half in range(CORES):
                cols = slice((d * CORES + half) * LANES, (d * CORES + half + 1) * LANES)
                part[half, s, d, u * body_rows:(u + 1) * body_rows, :] = prod[:body_rows, cols]
                tile = UNITS * body_rows
                if u == 0:
                    part[half, s, d, tile:tile + 8, :] = prod[body_rows:body_rows + 8, cols]
                else:
                    part[half, s, d, tile + u:tile + u + 1, :] = prod[body_rows:body_rows + 1, cols]
            pp_copy(s, u * DIRS + d).start()

        @pl.when(s < lastc)
        def _():
            for d in range(DIRS):
                w_copy(s + 1, u * DIRS + d).start()

    def ring(s, k):
        d, u = k % DIRS, k // DIRS
        rows = f_rows(u)
        pp_copy(s, k).wait_recv()

        @pl.when(s == 0)
        def _():
            part[core, s, d, rows, :] = part[core, s, d, rows, :] + part_in[s, d, rows, :]
            rs_copy(s, k).start()

        @pl.when(jnp.logical_and(s > 0, s < lastc))
        def _():
            rs_copy(s - 1, k).wait_recv()
            part[core, s, d, rows, :] = (part[core, s, d, rows, :] + part_in[s, d, rows, :]) + rs_in[s - 1, d, rows, :]
            rs_copy(s, k).start()

        @pl.when(s == lastc)
        def _():
            rs_copy(s - 1, k).wait_recv()
            total = (part[core, s, d, rows, :] + part_in[s, d, rows, :]) + rs_in[s - 1, d, rows, :]
            if u == UNITS - 1:
                total = jnp.concatenate([total, total[body_rows:, :]], axis=0)
            ag[0, d, h_rows(u), :] = total.astype(jnp.bfloat16)
            ag_copy(0, k).start()
            ap_copy(0, k).start()

    def ring_pair(s, u):
        for d in range(DIRS):
            ring(s, u * DIRS + d)

    @pl.loop(0, chips)
    def _(s):
        for u in range(UNITS):
            compute(s, u)
            if u > 0:
                ring_pair(s, u - 1)
            else:
                @pl.when(s > 0)
                def _():
                    ring_pair(s - 1, UNITS - 1)

    ring_pair(jnp.int32(lastc), UNITS - 1)

    @pl.loop(1, chips)
    def _(h):
        for k in range(n_k):
            ag_copy(h - 1, k).wait_recv()

            @pl.when(h < lastc)
            def _():
                ag_copy(h, k).start()

            ap_copy(h, k).start()

    @pl.loop(0, chips)
    def _(s):
        for k in range(n_k):
            pp_copy(s, k).wait_send()
            ap_copy(s, k).wait()

            @pl.when(s < lastc)
            def _():
                rs_copy(s, k).wait_send()
                ag_copy(s, k).wait_send()


def expand_kernel(chips, n_seq, seq_len, len_ref, ag, ag_pair, o_hbm, keep, alone, stage, sems):
    me = lax.axis_index("tp")
    z, core = me // CORES, lax.rem(me, CORES)
    body_rows = (n_seq - 1) * seq_len
    single = first_single(len_ref, n_seq)
    row = lax.broadcasted_iota(jnp.int32, (seq_len, LANES), 0)
    for s in range(n_seq):
        many = jnp.where(single == s, 0, len_ref[s])
        one = jnp.where(single == s, 1, 0)
        keep[s * seq_len:(s + 1) * seq_len, :] = jnp.where(row < many, 1.0, 0.0).astype(jnp.bfloat16)
        alone[s * 16:(s + 1) * 16, :] = jnp.where(row[:16] < one, 1.0, 0.0).astype(jnp.bfloat16)
    zero = jnp.bfloat16(0)

    def out_copy(h, d):
        chunk = lax.rem(z + chips - h, chips) if d == 0 else lax.rem(z + h, chips)
        wide = UNITS * CORES * LANES
        cols = pl.ds(pl.multiple_of((chunk * DIRS + d) * wide, wide), wide)
        return pltpu.make_async_copy(stage.at[h, d], o_hbm.at[:, cols], sems.at[h, d])

    @pl.loop(0, chips)
    def _(h):
        for d in range(DIRS):
            for near, ref in enumerate((ag, ag_pair)):
                side = core if near == 0 else 1 - core
                tile = ref[h, d, UNITS * body_rows:UNITS * body_rows + 16, :].astype(jnp.float32)
                for u in range(UNITS):
                    cols = pl.ds(pl.multiple_of((u * CORES + side) * LANES, LANES), LANES)
                    lone = jnp.broadcast_to(tile[u:u + 1, :], (16, LANES)).astype(jnp.bfloat16)
                    for s in range(n_seq):
                        pos = jnp.minimum(s - (single < s).astype(jnp.int32), n_seq - 2)
                        start = pl.multiple_of(u * body_rows + pos * seq_len, seq_len)
                        rows = ref[h, d, pl.ds(start, seq_len), :]
                        mask = keep[s * seq_len:(s + 1) * seq_len, :]
                        first = jnp.where(alone[s * 16:(s + 1) * 16, :] > zero, lone, zero)
                        base = s * seq_len
                        stage[h, d, base:base + 16, cols] = jnp.where(mask[:16] > zero, rows[:16], first)
                        stage[h, d, base + 16:base + seq_len, cols] = jnp.where(mask[16:] > zero, rows[16:], zero)
            out_copy(h, d).start()

    @pl.loop(0, chips)
    def _(h):
        for d in range(DIRS):
            out_copy(h, d).wait()


def solution(mesh):
    chips = mesh.shape["tp"] // CORES

    def local_part(x_loc, w_loc, lengths):
        tokens, depth = x_loc.shape
        columns = w_loc.shape[1]
        n_seq = lengths.shape[0]
        seq_len = tokens // n_seq
        body_rows = (n_seq - 1) * seq_len
        n_k = DIRS * UNITS
        assert columns == chips * DIRS * UNITS * CORES * LANES
        f_tall, h_tall = UNITS * body_rows + 8, UNITS * body_rows + 16
        dma = pltpu.SemaphoreType.DMA
        held = pltpu.VMEM((chips, DIRS, h_tall, LANES), jnp.bfloat16)
        vmem = pl.BlockSpec(memory_space=pltpu.VMEM)
        smem = pl.BlockSpec(memory_space=pltpu.SMEM)
        hbm = pl.BlockSpec(memory_space=pl.ANY)
        near, far = pl.pallas_call(
            functools.partial(reduce_kernel, chips, n_seq, seq_len),
            out_shape=(held, held),
            in_specs=[smem, hbm, hbm],
            out_specs=(vmem, vmem),
            scratch_shapes=[
                pltpu.VMEM((tokens, depth), jnp.bfloat16),
                pltpu.VMEM((body_rows + 16, depth), jnp.bfloat16),
                pltpu.VMEM((UNITS, depth, DIRS * CORES * LANES), jnp.bfloat16),
                pltpu.VMEM((CORES, chips, DIRS, f_tall, LANES), jnp.float32),
                pltpu.VMEM((chips, DIRS, f_tall, LANES), jnp.float32),
                pltpu.VMEM((chips - 1, DIRS, f_tall, LANES), jnp.float32),
                dma,
                dma((n_k,)),
                dma((chips, n_k)), dma((chips, n_k)),
                dma((chips - 1, n_k)), dma((chips - 1, n_k)),
                dma((chips - 1, n_k)), dma((chips - 1, n_k)),
                dma((chips, n_k)), dma((chips, n_k)),
            ],
            compiler_params=pltpu.CompilerParams(
                collective_id=0, has_side_effects=True, vmem_limit_bytes=48 * 1024 * 1024),
            name="reduce_gather",
        )(lengths, x_loc, w_loc)
        return pl.pallas_call(
            functools.partial(expand_kernel, chips, n_seq, seq_len),
            out_shape=jax.ShapeDtypeStruct((tokens, columns), jnp.bfloat16),
            in_specs=[smem, vmem, vmem],
            out_specs=hbm,
            scratch_shapes=[
                pltpu.VMEM((tokens, LANES), jnp.bfloat16),
                pltpu.VMEM((n_seq * 16, LANES), jnp.bfloat16),
                pltpu.VMEM((chips, DIRS, tokens, UNITS * CORES * LANES), jnp.bfloat16),
                dma((chips, DIRS)),
            ],
            compiler_params=pltpu.CompilerParams(vmem_limit_bytes=32 * 1024 * 1024),
            name="expand_rows",
        )(lengths, near, far)

    return jax.shard_map(local_part, mesh=mesh, in_specs=(P("data", "tp"), P("tp", None), P("data")), out_specs=P("data", None), check_vma=False)
```

```python
import functools

import jax
import jax.numpy as jnp
from jax import lax
from jax.experimental import pallas as pl
from jax.experimental.pallas import tpu as pltpu
from jax.sharding import PartitionSpec as P

MESH = pl.DeviceIdType.MESH
LANES = 128
CORES = 2
DIRS = 2
UNITS = 3
STEPS = 127 * 256


def first_single(len_ref, n_seq):
    slot = jnp.int32(n_seq - 1)
    for s in reversed(range(n_seq - 1)):
        slot = jnp.where(len_ref[s] == 1, jnp.int32(s), slot)
    return slot


def split_sum(total, rows):
    high = total.astype(jnp.bfloat16)
    wide = high.astype(jnp.float32)
    left = jnp.round((total - wide) / jnp.where(wide == 0.0, 1.0, wide) * STEPS)
    low = left[:rows // 2] * 256.0 + left[rows // 2:]
    return high, low.astype(jnp.int32).astype(jnp.int16)


def join_sum(high, low):
    pair = low.astype(jnp.int32).astype(jnp.float32)
    first = jnp.round(pair * (1.0 / 256.0))
    left = jnp.concatenate([first, pair - first * 256.0], axis=0)
    wide = high.astype(jnp.float32)
    return wide + wide * (left * (1.0 / STEPS))


def split_lone(total):
    high = total.astype(jnp.bfloat16).astype(jnp.float32)
    return jnp.concatenate([high, total - high], axis=0).astype(jnp.bfloat16)


def join_lone(both):
    both = both.astype(jnp.float32)
    return both[:8] + both[8:]


def reduce_kernel(
    chips, n_seq, seq_len,
    len_ref, x_hbm, w_hbm, ag, ag_pair,
    x_raw, xc, wbuf, part, part_in, tx_hi, tx_lo, rx_hi, rx_lo,
    x_sem, w_sem, pp_send, pp_recv, hi_send, hi_recv, lo_send, lo_recv, ag_send, ag_recv, ap_send, ap_recv,
):
    me = lax.axis_index("tp")
    z, core = me // CORES, lax.rem(me, CORES)
    nxt = lax.rem(z + 1, chips) * CORES + core
    prv = lax.rem(z + chips - 1, chips) * CORES + core
    mate = z * CORES + (1 - core)
    towards = (nxt, prv)
    body_rows = (n_seq - 1) * seq_len
    lastc = chips - 1
    n_k = DIRS * UNITS

    def chunk_of(s, d):
        if d == 0:
            return lax.rem(z + (2 * chips - 1) - s, chips)
        return lax.rem(z + 1 + s, chips)

    def w_copy(s, k):
        d, u = k % DIRS, k // DIRS
        col = ((chunk_of(s, d) * DIRS + d) * UNITS + u) * (CORES * LANES)
        col = pl.multiple_of(col, CORES * LANES)
        return pltpu.make_async_copy(w_hbm.at[:, pl.ds(col, CORES * LANES)], wbuf.at[u, :, pl.ds(d * CORES * LANES, CORES * LANES)], w_sem.at[k])

    def f_rows(u):
        return pl.ds(u * body_rows, body_rows + (8 if u == UNITS - 1 else 0))

    def h_rows(u):
        return pl.ds(u * body_rows, body_rows + (16 if u == UNITS - 1 else 0))

    def b_rows(u):
        return pl.ds(u * body_rows, body_rows)

    def l_rows(u):
        return pl.ds(u * (body_rows // 2), body_rows // 2)

    f_tail, h_tail = pl.ds(UNITS * body_rows, 8), pl.ds(UNITS * body_rows, 16)

    x_copy = pltpu.make_async_copy(x_hbm, x_raw, x_sem)
    x_copy.start()
    for k in range(n_k):
        w_copy(0, k).start()

    barrier = pltpu.get_barrier_semaphore()
    for peer in (mate, nxt, prv):
        pl.semaphore_signal(barrier, inc=1, device_id={"tp": peer}, device_id_type=MESH)

    single = first_single(len_ref, n_seq)
    x_copy.wait()
    def x_rows(slot, count):
        return x_raw[slot * seq_len:slot * seq_len + count, :]

    for p in range(n_seq - 1):
        xc[p * seq_len:(p + 1) * seq_len, :] = jnp.where(single <= p, x_rows(p + 1, seq_len), x_rows(p, seq_len))
    lone = x_rows(n_seq - 1, 16)
    for s in range(n_seq - 1):
        lone = jnp.where(single == s, x_rows(s, 16), lone)
    xc[body_rows:body_rows + 16, :] = lone
    pl.semaphore_wait(barrier, 3)

    def pp_copy(s, k):
        d, u = k % DIRS, k // DIRS
        return pltpu.make_async_remote_copy(
            src_ref=part.at[1 - core, s, d, f_rows(u)], dst_ref=part_in.at[s, d, f_rows(u)],
            send_sem=pp_send.at[s, k], recv_sem=pp_recv.at[s, k], device_id={"tp": mate}, device_id_type=MESH)

    def hi_copy(s, k):
        d, u = k % DIRS, k // DIRS
        return pltpu.make_async_remote_copy(
            src_ref=tx_hi.at[s, d, h_rows(u)], dst_ref=rx_hi.at[s, d, h_rows(u)],
            send_sem=hi_send.at[s, k], recv_sem=hi_recv.at[s, k], device_id={"tp": towards[d]}, device_id_type=MESH)

    def lo_copy(s, k):
        d, u = k % DIRS, k // DIRS
        return pltpu.make_async_remote_copy(
            src_ref=tx_lo.at[s, d, l_rows(u)], dst_ref=rx_lo.at[s, d, l_rows(u)],
            send_sem=lo_send.at[s, k], recv_sem=lo_recv.at[s, k], device_id={"tp": towards[d]}, device_id_type=MESH)

    def ag_copy(h, k):
        d, u = k % DIRS, k // DIRS
        return pltpu.make_async_remote_copy(
            src_ref=ag.at[h, d, h_rows(u)], dst_ref=ag.at[h + 1, d, h_rows(u)],
            send_sem=ag_send.at[h, k], recv_sem=ag_recv.at[h, k], device_id={"tp": towards[d]}, device_id_type=MESH)

    def ap_copy(h, k):
        d, u = k % DIRS, k // DIRS
        return pltpu.make_async_remote_copy(
            src_ref=ag.at[h, d, h_rows(u)], dst_ref=ag_pair.at[h, d, h_rows(u)],
            send_sem=ap_send.at[h, k], recv_sem=ap_recv.at[h, k], device_id={"tp": mate}, device_id_type=MESH)

    def compute(s, u):
        for d in range(DIRS):
            w_copy(s, u * DIRS + d).wait()
        prod = jnp.dot(xc[...], wbuf[u], preferred_element_type=jnp.float32)
        for d in range(DIRS):
            for half in range(CORES):
                cols = slice((d * CORES + half) * LANES, (d * CORES + half + 1) * LANES)
                part[half, s, d, u * body_rows:(u + 1) * body_rows, :] = prod[:body_rows, cols]
                tile = UNITS * body_rows
                if u == 0:
                    part[half, s, d, tile:tile + 8, :] = prod[body_rows:body_rows + 8, cols]
                else:
                    part[half, s, d, tile + u:tile + u + 1, :] = prod[body_rows:body_rows + 1, cols]
            pp_copy(s, u * DIRS + d).start()

        @pl.when(s < lastc)
        def _():
            for d in range(DIRS):
                w_copy(s + 1, u * DIRS + d).start()

    def ring(s, k):
        d, u = k % DIRS, k // DIRS
        rows, last = b_rows(u), u == UNITS - 1

        def here(where):
            return part[core, s, d, where, :] + part_in[s, d, where, :]

        def arrived():
            return join_sum(rx_hi[s - 1, d, rows, :], rx_lo[s - 1, d, l_rows(u), :])

        def arrived_lone():
            return join_lone(rx_hi[s - 1, d, h_tail, :])

        def send(total, lone):
            tx_hi[s, d, rows, :], tx_lo[s, d, l_rows(u), :] = split_sum(total, body_rows)
            if last:
                tx_hi[s, d, h_tail, :] = split_lone(lone)
            hi_copy(s, k).start()
            lo_copy(s, k).start()

        pp_copy(s, k).wait_recv()

        @pl.when(s == 0)
        def _():
            send(here(rows), here(f_tail) if last else None)

        @pl.when(jnp.logical_and(s > 0, s < lastc))
        def _():
            hi_copy(s - 1, k).wait_recv()
            lo_copy(s - 1, k).wait_recv()
            send(here(rows) + arrived(), here(f_tail) + arrived_lone() if last else None)

        @pl.when(s == lastc)
        def _():
            hi_copy(s - 1, k).wait_recv()
            lo_copy(s - 1, k).wait_recv()
            ag[0, d, rows, :] = (here(rows) + arrived()).astype(jnp.bfloat16)
            if last:
                lone = here(f_tail) + arrived_lone()
                ag[0, d, h_tail, :] = jnp.concatenate([lone, lone], axis=0).astype(jnp.bfloat16)
            ag_copy(0, k).start()
            ap_copy(0, k).start()

    def ring_pair(s, u):
        for d in range(DIRS):
            ring(s, u * DIRS + d)

    @pl.loop(0, chips)
    def _(s):
        for u in range(UNITS):
            compute(s, u)
            if u > 0:
                ring_pair(s, u - 1)
            else:
                @pl.when(s > 0)
                def _():
                    ring_pair(s - 1, UNITS - 1)

    ring_pair(jnp.int32(lastc), UNITS - 1)

    @pl.loop(1, chips)
    def _(h):
        for k in range(n_k):
            ag_copy(h - 1, k).wait_recv()

            @pl.when(h < lastc)
            def _():
                ag_copy(h, k).start()

            ap_copy(h, k).start()

    @pl.loop(0, chips)
    def _(s):
        for k in range(n_k):
            pp_copy(s, k).wait_send()
            ap_copy(s, k).wait()

            @pl.when(s < lastc)
            def _():
                hi_copy(s, k).wait_send()
                lo_copy(s, k).wait_send()
                ag_copy(s, k).wait_send()


def expand_kernel(chips, n_seq, seq_len, len_ref, ag, ag_pair, o_hbm, keep, alone, stage, sems):
    me = lax.axis_index("tp")
    z, core = me // CORES, lax.rem(me, CORES)
    body_rows = (n_seq - 1) * seq_len
    single = first_single(len_ref, n_seq)
    row = lax.broadcasted_iota(jnp.int32, (seq_len, LANES), 0)
    for s in range(n_seq):
        many = jnp.where(single == s, 0, len_ref[s])
        one = jnp.where(single == s, 1, 0)
        keep[s * seq_len:(s + 1) * seq_len, :] = jnp.where(row < many, 1.0, 0.0).astype(jnp.bfloat16)
        alone[s * 16:(s + 1) * 16, :] = jnp.where(row[:16] < one, 1.0, 0.0).astype(jnp.bfloat16)
    zero = jnp.bfloat16(0)

    def out_copy(h, d):
        chunk = lax.rem(z + chips - h, chips) if d == 0 else lax.rem(z + h, chips)
        wide = UNITS * CORES * LANES
        cols = pl.ds(pl.multiple_of((chunk * DIRS + d) * wide, wide), wide)
        return pltpu.make_async_copy(stage.at[h, d], o_hbm.at[:, cols], sems.at[h, d])

    @pl.loop(0, chips)
    def _(h):
        for d in range(DIRS):
            for near, ref in enumerate((ag, ag_pair)):
                side = core if near == 0 else 1 - core
                tile = ref[h, d, UNITS * body_rows:UNITS * body_rows + 16, :].astype(jnp.float32)
                for u in range(UNITS):
                    cols = pl.ds(pl.multiple_of((u * CORES + side) * LANES, LANES), LANES)
                    lone = jnp.broadcast_to(tile[u:u + 1, :], (16, LANES)).astype(jnp.bfloat16)
                    for s in range(n_seq):
                        pos = jnp.minimum(s - (single < s).astype(jnp.int32), n_seq - 2)
                        start = pl.multiple_of(u * body_rows + pos * seq_len, seq_len)
                        rows = ref[h, d, pl.ds(start, seq_len), :]
                        mask = keep[s * seq_len:(s + 1) * seq_len, :]
                        first = jnp.where(alone[s * 16:(s + 1) * 16, :] > zero, lone, zero)
                        base = s * seq_len
                        stage[h, d, base:base + 16, cols] = jnp.where(mask[:16] > zero, rows[:16], first)
                        stage[h, d, base + 16:base + seq_len, cols] = jnp.where(mask[16:] > zero, rows[16:], zero)
            out_copy(h, d).start()

    @pl.loop(0, chips)
    def _(h):
        for d in range(DIRS):
            out_copy(h, d).wait()


def solution(mesh):
    chips = mesh.shape["tp"] // CORES

    def local_part(x_loc, w_loc, lengths):
        tokens, depth = x_loc.shape
        columns = w_loc.shape[1]
        n_seq = lengths.shape[0]
        seq_len = tokens // n_seq
        body_rows = (n_seq - 1) * seq_len
        n_k = DIRS * UNITS
        assert columns == chips * DIRS * UNITS * CORES * LANES
        f_tall, h_tall = UNITS * body_rows + 8, UNITS * body_rows + 16
        dma = pltpu.SemaphoreType.DMA
        held = pltpu.VMEM((chips, DIRS, h_tall, LANES), jnp.bfloat16)
        vmem = pl.BlockSpec(memory_space=pltpu.VMEM)
        smem = pl.BlockSpec(memory_space=pltpu.SMEM)
        hbm = pl.BlockSpec(memory_space=pl.ANY)
        near, far = pl.pallas_call(
            functools.partial(reduce_kernel, chips, n_seq, seq_len),
            out_shape=(held, held),
            in_specs=[smem, hbm, hbm],
            out_specs=(vmem, vmem),
            scratch_shapes=[
                pltpu.VMEM((tokens, depth), jnp.bfloat16),
                pltpu.VMEM((body_rows + 16, depth), jnp.bfloat16),
                pltpu.VMEM((UNITS, depth, DIRS * CORES * LANES), jnp.bfloat16),
                pltpu.VMEM((CORES, chips, DIRS, f_tall, LANES), jnp.float32),
                pltpu.VMEM((chips, DIRS, f_tall, LANES), jnp.float32),
                pltpu.VMEM((chips - 1, DIRS, h_tall, LANES), jnp.bfloat16),
                pltpu.VMEM((chips - 1, DIRS, UNITS * body_rows // 2, LANES), jnp.int16),
                pltpu.VMEM((chips - 1, DIRS, h_tall, LANES), jnp.bfloat16),
                pltpu.VMEM((chips - 1, DIRS, UNITS * body_rows // 2, LANES), jnp.int16),
                dma,
                dma((n_k,)),
                dma((chips, n_k)), dma((chips, n_k)),
                dma((chips - 1, n_k)), dma((chips - 1, n_k)),
                dma((chips - 1, n_k)), dma((chips - 1, n_k)),
                dma((chips - 1, n_k)), dma((chips - 1, n_k)),
                dma((chips, n_k)), dma((chips, n_k)),
            ],
            compiler_params=pltpu.CompilerParams(
                collective_id=0, has_side_effects=True, vmem_limit_bytes=48 * 1024 * 1024),
            name="reduce_gather",
        )(lengths, x_loc, w_loc)
        return pl.pallas_call(
            functools.partial(expand_kernel, chips, n_seq, seq_len),
            out_shape=jax.ShapeDtypeStruct((tokens, columns), jnp.bfloat16),
            in_specs=[smem, vmem, vmem],
            out_specs=hbm,
            scratch_shapes=[
                pltpu.VMEM((tokens, LANES), jnp.bfloat16),
                pltpu.VMEM((n_seq * 16, LANES), jnp.bfloat16),
                pltpu.VMEM((chips, DIRS, tokens, UNITS * CORES * LANES), jnp.bfloat16),
                dma((chips, DIRS)),
            ],
            compiler_params=pltpu.CompilerParams(vmem_limit_bytes=32 * 1024 * 1024),
            name="expand_rows",
        )(lengths, near, far)

    return jax.shard_map(local_part, mesh=mesh, in_specs=(P("data", "tp"), P("tp", None), P("data")), out_specs=P("data", None), check_vma=False)
```

```python
import functools

import jax
import jax.numpy as jnp
from jax import lax
from jax.experimental import pallas as pl
from jax.experimental.pallas import tpu as pltpu
from jax.sharding import PartitionSpec as P

MESH = pl.DeviceIdType.MESH
LANES = 128
CORES = 2
WAYS = 2
UNITS = 3
SLOTS = UNITS * WAYS
BLOCK = CORES * WAYS * LANES
LONE = UNITS * WAYS - 1
STEPS = 127 * 256


def first_single(len_ref, n_seq):
    slot = jnp.int32(n_seq - 1)
    for s in reversed(range(n_seq - 1)):
        slot = jnp.where(len_ref[s] == 1, jnp.int32(s), slot)
    return slot


def split_sum(total, rows):
    high = total.astype(jnp.bfloat16)
    wide = high.astype(jnp.float32)
    left = jnp.round((total - wide) / jnp.where(wide == 0.0, 1.0, wide) * STEPS)
    low = left[:rows // 2] * 256.0 + left[rows // 2:]
    return high, low.astype(jnp.int32).astype(jnp.int16)


def join_sum(high, low):
    pair = low.astype(jnp.int32).astype(jnp.float32)
    first = jnp.round(pair * (1.0 / 256.0))
    left = jnp.concatenate([first, pair - first * 256.0], axis=0)
    wide = high.astype(jnp.float32)
    return wide + wide * (left * (1.0 / STEPS))


def split_lone(total):
    high = total.astype(jnp.bfloat16).astype(jnp.float32)
    return jnp.concatenate([high, total - high], axis=0).astype(jnp.bfloat16)


def join_lone(both):
    both = both.astype(jnp.float32)
    return both[:8] + both[8:]


class Rows:
    def __init__(self, tall, tail):
        self.tall, self.tail = tall, tail
        self.total = SLOTS * tall + tail

    def lone(self):
        return pl.ds(LONE * self.tall, self.tail)

    def tile(self, u, d):
        i = u * WAYS + d
        return pl.ds(i * self.tall + (self.tail if i >= LONE else 0), self.tall)

    def pair(self, u):
        return pl.ds(u * WAYS * self.tall, WAYS * self.tall + (self.tail if u == UNITS - 1 else 0))

    def half(self, u, d, lone=True):
        i = u * WAYS + d
        more = self.tail if (u == UNITS - 1 and lone) else 0
        start = i * self.tall + (self.tail if (i >= LONE and not lone) else 0)
        return pl.ds(start, self.tall + more)


def reduce_kernel(
    chips, n_seq, seq_len,
    len_ref, x_hbm, w_hbm, ag, ag_pair,
    x_raw, xc, wbuf, part, part_in, tx_hi, tx_lo, rx_hi, rx_lo,
    x_sem, w_sem, pp_send, pp_recv, hi_send, hi_recv, lo_send, lo_recv, ag_send, ag_recv, ap_send, ap_recv,
):
    me = lax.axis_index("tp")
    z, core = me // CORES, lax.rem(me, CORES)
    nxt = lax.rem(z + 1, chips) * CORES + core
    prv = lax.rem(z + chips - 1, chips) * CORES + core
    mate = z * CORES + (1 - core)
    body_rows = (n_seq - 1) * seq_len
    far = chips // 2
    last = UNITS - 1
    wide, packed, low = Rows(body_rows, 8), Rows(body_rows, 16), Rows(body_rows // 2, 0)

    def place(t, side):
        return jnp.where(t == 0, 0, jnp.where(t == far, 2 * far - 1, 2 * t - 1 + side))

    def w_copy(t, u, side):
        chunk = lax.rem(z + chips + (t - far if side == 0 else far - t), chips)
        col = pl.multiple_of((chunk * UNITS + u) * BLOCK, BLOCK)
        b = u * WAYS + side
        return pltpu.make_async_copy(w_hbm.at[:, pl.ds(col, BLOCK)], wbuf.at[b], w_sem.at[b])

    x_copy = pltpu.make_async_copy(x_hbm, x_raw, x_sem)
    x_copy.start()
    w_copy(0, 0, 0).start()

    barrier = pltpu.get_barrier_semaphore()
    for peer in (mate, nxt, prv):
        pl.semaphore_signal(barrier, inc=1, device_id={"tp": peer}, device_id_type=MESH)

    single = first_single(len_ref, n_seq)
    x_copy.wait()
    for u in range(1, UNITS):
        w_copy(0, u, 0).start()
    for u in range(UNITS):
        w_copy(1, u, 1).start()

    def x_rows(slot, count):
        return x_raw[slot * seq_len:slot * seq_len + count, :]

    for p in range(n_seq - 1):
        xc[p * seq_len:(p + 1) * seq_len, :] = jnp.where(single <= p, x_rows(p + 1, seq_len), x_rows(p, seq_len))
    lone = x_rows(n_seq - 1, 16)
    for s in range(n_seq - 1):
        lone = jnp.where(single == s, x_rows(s, 16), lone)
    xc[body_rows:body_rows + 16, :] = lone
    pl.semaphore_wait(barrier, 3)

    def pp_copy(t, u, side):
        q = place(t, side)
        return pltpu.make_async_remote_copy(
            src_ref=part.at[1 - core, q, wide.pair(u)], dst_ref=part_in.at[q, wide.pair(u)],
            send_sem=pp_send.at[q, u], recv_sem=pp_recv.at[q, u], device_id={"tp": mate}, device_id_type=MESH)

    def rs_copies(t, u, side, far_end):
        peer = prv if side == 0 else nxt
        copies = []
        for tx, rx, ss, rs, rows in ((tx_hi, rx_hi, hi_send, hi_recv, packed), (tx_lo, rx_lo, lo_send, lo_recv, low)):
            where = rows.half(u, side) if far_end else rows.pair(u)
            copies.append(pltpu.make_async_remote_copy(
                src_ref=tx.at[side, t, where], dst_ref=rx.at[side, t, where],
                send_sem=ss.at[side, t, u], recv_sem=rs.at[side, t, u], device_id={"tp": peer}, device_id_type=MESH))
        return copies

    def ag_where(u, way, half):
        return packed.half(u, way, lone=way == 0) if half else packed.pair(u)

    def slot_of(h, way):
        return h if way == 0 else lax.rem(2 * far - h, 2 * far)

    def ag_copy(h, u, way, half):
        where = ag_where(u, way, half)
        return pltpu.make_async_remote_copy(
            src_ref=ag.at[slot_of(h, way), where], dst_ref=ag.at[slot_of(h + 1, way), where],
            send_sem=ag_send.at[way, h, u], recv_sem=ag_recv.at[way, h, u],
            device_id={"tp": nxt if way == 0 else prv}, device_id_type=MESH)

    def ap_copy(h, u, way, half=False):
        where = ag_where(u, way, half)
        return pltpu.make_async_remote_copy(
            src_ref=ag.at[slot_of(h, way), where], dst_ref=ag_pair.at[slot_of(h, way), where],
            send_sem=ap_send.at[way, h, u], recv_sem=ap_recv.at[way, h, u], device_id={"tp": mate}, device_id_type=MESH)

    def compute(t, u, side):
        q = place(t, side)
        w_copy(t, u, side).wait()
        prod = jnp.dot(xc[...], wbuf[u * WAYS + side], preferred_element_type=jnp.float32)
        for d in range(WAYS):
            i = u * WAYS + d
            for half in range(CORES):
                cols = slice((d * CORES + half) * LANES, (d * CORES + half + 1) * LANES)
                part[half, q, wide.tile(u, d), :] = prod[:body_rows, cols]
                tile = LONE * body_rows
                if i == 0:
                    part[half, q, tile:tile + 8, :] = prod[body_rows:body_rows + 8, cols]
                else:
                    part[half, q, tile + i:tile + i + 1, :] = prod[body_rows:body_rows + 1, cols]
        pp_copy(t, u, side).start()

        @pl.when(t < (far if side == 0 else far - 1))
        def _():
            w_copy(t + 1, u, side).start()

    def ring(t, u, side):
        q = place(t, side)
        parity = lax.rem(lax.broadcasted_iota(jnp.int32, (8, LANES), 0), WAYS)

        def here(where):
            return part[core, q, where, :] + part_in[q, where, :]

        def arrived(side_, d):
            return join_sum(rx_hi[side_, t - 1, packed.tile(u, d), :], rx_lo[side_, t - 1, low.tile(u, d), :])

        def arrived_lone(side_):
            return join_lone(rx_hi[side_, t - 1, packed.lone(), :])

        def put(side_, d, total):
            tx_hi[side_, t, packed.tile(u, d), :], tx_lo[side_, t, low.tile(u, d), :] = split_sum(total, body_rows)

        def put_lone(side_, total):
            tx_hi[side_, t, packed.lone(), :] = split_lone(total)

        if side == 0:
            @pl.when(t == 0)
            def _():
                pp_copy(t, u, side).wait_recv()
                for d in range(WAYS):
                    put(d, d, here(wide.tile(u, d)))
                    if u == last:
                        put_lone(d, here(wide.lone()))
                    for copy in rs_copies(0, u, d, True):
                        copy.start()

        @pl.when(t == 1)
        def _():
            pp_copy(t, u, side).wait_recv()
            put(side, 1 - side, here(wide.tile(u, 1 - side)))
            for copy in rs_copies(0, u, side, True):
                copy.wait_recv()
            put(side, side, here(wide.tile(u, side)) + arrived(side, side))
            if u == last:
                put_lone(side, here(wide.lone()) + jnp.where(parity == side, arrived_lone(side), 0.0))
            for copy in rs_copies(1, u, side, False):
                copy.start()

        @pl.when(jnp.logical_and(t > 1, t < far))
        def _():
            pp_copy(t, u, side).wait_recv()
            for copy in rs_copies(t - 1, u, side, False):
                copy.wait_recv()
            for d in range(WAYS):
                put(side, d, here(wide.tile(u, d)) + arrived(side, d))
            if u == last:
                put_lone(side, here(wide.lone()) + arrived_lone(side))
            for copy in rs_copies(t, u, side, False):
                copy.start()

        if side == 0:
            @pl.when(t == far)
            def _():
                pp_copy(t, u, side).wait_recv()
                for way in range(WAYS):
                    for copy in rs_copies(t - 1, u, way, False):
                        copy.wait_recv()
                for d in range(WAYS):
                    total = (here(wide.tile(u, d)) + arrived(0, d)) + arrived(1, d)
                    ag[0, packed.tile(u, d), :] = total.astype(jnp.bfloat16)
                if u == last:
                    total = (here(wide.lone()) + arrived_lone(0)) + arrived_lone(1)
                    ag[0, packed.lone(), :] = jnp.concatenate([total, total], axis=0).astype(jnp.bfloat16)
                for way in range(WAYS):
                    ag_copy(0, u, way, False).start()
                ap_copy(0, u, 0).start()

    turns = [(u, side) for u in range(UNITS) for side in range(WAYS)]

    @pl.loop(0, far + 1)
    def _(t):
        for i, (u, side) in enumerate(turns):
            if side == 0:
                compute(t, u, side)
            else:
                @pl.when(jnp.logical_and(t > 0, t < far))
                def _():
                    compute(t, u, side)
            if i >= 2:
                ring(t, *turns[i - 2])
            else:
                @pl.when(t > 0)
                def _():
                    ring(t - 1, *turns[i - 2])

    ring(jnp.int32(far), *turns[-2])

    def pass_on(h, half):
        for u in range(UNITS):
            for way in range(WAYS):
                ag_copy(h - 1, u, way, False).wait_recv()
                ag_copy(h, u, way, half).start()
                ap_copy(h, u, way).start()

    @pl.loop(1, far - 1)
    def _(h):
        pass_on(h, False)

    pass_on(far - 1, True)
    for u in range(UNITS):
        for way in range(WAYS):
            ag_copy(far - 1, u, way, True).wait_recv()
            ap_copy(far, u, way, True).start()

    for u in range(UNITS):
        ap_copy(0, u, 0).wait()
        for side in range(WAYS):
            for copy in rs_copies(0, u, side, True):
                copy.wait_send()
            ag_copy(far - 1, u, side, True).wait_send()
            ap_copy(far, u, side, True).wait()

    @pl.loop(0, 2 * far)
    def _(q):
        for u in range(UNITS):
            pltpu.make_async_remote_copy(
                src_ref=part.at[1 - core, q, wide.pair(u)], dst_ref=part_in.at[q, wide.pair(u)],
                send_sem=pp_send.at[q, u], recv_sem=pp_recv.at[q, u], device_id={"tp": mate}, device_id_type=MESH).wait_send()

    @pl.loop(1, far)
    def _(t):
        for u in range(UNITS):
            for side in range(WAYS):
                for copy in rs_copies(t, u, side, False):
                    copy.wait_send()
                ag_copy(t - 1, u, side, False).wait_send()
                ap_copy(t, u, side).wait()


def expand_kernel(chips, n_seq, seq_len, len_ref, ag, ag_pair, o_hbm, keep, alone, stage, sems):
    me = lax.axis_index("tp")
    z, core = me // CORES, lax.rem(me, CORES)
    body_rows = (n_seq - 1) * seq_len
    packed = Rows(body_rows, 16)
    single = first_single(len_ref, n_seq)
    row = lax.broadcasted_iota(jnp.int32, (seq_len, LANES), 0)
    for s in range(n_seq):
        many = jnp.where(single == s, 0, len_ref[s])
        one = jnp.where(single == s, 1, 0)
        keep[s * seq_len:(s + 1) * seq_len, :] = jnp.where(row < many, 1.0, 0.0).astype(jnp.bfloat16)
        alone[s * 16:(s + 1) * 16, :] = jnp.where(row[:16] < one, 1.0, 0.0).astype(jnp.bfloat16)
    zero = jnp.bfloat16(0)

    def out_copy(slot):
        cols = pl.ds(pl.multiple_of(lax.rem(z + chips - slot, chips) * (UNITS * BLOCK), UNITS * BLOCK), UNITS * BLOCK)
        return pltpu.make_async_copy(stage.at[slot], o_hbm.at[:, cols], sems.at[slot])

    @pl.loop(0, chips)
    def _(slot):
        for near, ref in enumerate((ag, ag_pair)):
            side = core if near == 0 else 1 - core
            tail = ref[slot, packed.lone(), :].astype(jnp.float32)
            for i in range(SLOTS):
                cols = pl.ds(pl.multiple_of((i * CORES + side) * LANES, LANES), LANES)
                lone = jnp.broadcast_to(tail[i:i + 1, :], (16, LANES)).astype(jnp.bfloat16)
                top = packed.tile(i // WAYS, i % WAYS).start
                for s in range(n_seq):
                    pos = jnp.minimum(s - (single < s).astype(jnp.int32), n_seq - 2)
                    rows = ref[slot, pl.ds(pl.multiple_of(top + pos * seq_len, 16), seq_len), :]
                    mask = keep[s * seq_len:(s + 1) * seq_len, :]
                    first = jnp.where(alone[s * 16:(s + 1) * 16, :] > zero, lone, zero)
                    base = s * seq_len
                    stage[slot, base:base + 16, cols] = jnp.where(mask[:16] > zero, rows[:16], first)
                    stage[slot, base + 16:base + seq_len, cols] = jnp.where(mask[16:] > zero, rows[16:], zero)
        out_copy(slot).start()

    @pl.loop(0, chips)
    def _(slot):
        out_copy(slot).wait()


def solution(mesh):
    chips = mesh.shape["tp"] // CORES

    def local_part(x_loc, w_loc, lengths):
        tokens, depth = x_loc.shape
        columns = w_loc.shape[1]
        n_seq = lengths.shape[0]
        seq_len = tokens // n_seq
        body_rows = (n_seq - 1) * seq_len
        far = chips // 2
        assert columns == chips * UNITS * BLOCK and chips == 2 * far and far >= 3
        wide, packed, low = Rows(body_rows, 8), Rows(body_rows, 16), Rows(body_rows // 2, 0)
        dma = pltpu.SemaphoreType.DMA
        held = pltpu.VMEM((chips, packed.total, LANES), jnp.bfloat16)
        vmem = pl.BlockSpec(memory_space=pltpu.VMEM)
        smem = pl.BlockSpec(memory_space=pltpu.SMEM)
        hbm = pl.BlockSpec(memory_space=pl.ANY)
        high = pltpu.VMEM((WAYS, far, packed.total, LANES), jnp.bfloat16)
        lows = pltpu.VMEM((WAYS, far, low.total, LANES), jnp.int16)
        hops = dma((WAYS, far, UNITS))
        near, others = pl.pallas_call(
            functools.partial(reduce_kernel, chips, n_seq, seq_len),
            out_shape=(held, held),
            in_specs=[smem, hbm, hbm],
            out_specs=(vmem, vmem),
            scratch_shapes=[
                pltpu.VMEM((tokens, depth), jnp.bfloat16),
                pltpu.VMEM((body_rows + 16, depth), jnp.bfloat16),
                pltpu.VMEM((SLOTS, depth, BLOCK), jnp.bfloat16),
                pltpu.VMEM((CORES, chips, wide.total, LANES), jnp.float32),
                pltpu.VMEM((chips, wide.total, LANES), jnp.float32),
                high, lows, high, lows,
                dma,
                dma((SLOTS,)),
                dma((chips, UNITS)), dma((chips, UNITS)),
                hops, hops, hops, hops, hops, hops,
                dma((WAYS, far + 1, UNITS)), dma((WAYS, far + 1, UNITS)),
            ],
            compiler_params=pltpu.CompilerParams(
                collective_id=0, has_side_effects=True, vmem_limit_bytes=52 * 1024 * 1024),
            name="reduce_gather",
        )(lengths, x_loc, w_loc)
        return pl.pallas_call(
            functools.partial(expand_kernel, chips, n_seq, seq_len),
            out_shape=jax.ShapeDtypeStruct((tokens, columns), jnp.bfloat16),
            in_specs=[smem, vmem, vmem],
            out_specs=hbm,
            scratch_shapes=[
                pltpu.VMEM((tokens, LANES), jnp.bfloat16),
                pltpu.VMEM((n_seq * 16, LANES), jnp.bfloat16),
                pltpu.VMEM((chips, tokens, UNITS * BLOCK), jnp.bfloat16),
                dma((chips,)),
            ],
            compiler_params=pltpu.CompilerParams(vmem_limit_bytes=32 * 1024 * 1024),
            name="expand_rows",
        )(lengths, near, others)

    return jax.shard_map(local_part, mesh=mesh, in_specs=(P("data", "tp"), P("tp", None), P("data")), out_specs=P("data", None), check_vma=False)
```

```python
import functools

import jax
import jax.numpy as jnp
from jax import lax
from jax.experimental import pallas as pl
from jax.experimental.pallas import tpu as pltpu
from jax.sharding import PartitionSpec as P

MESH = pl.DeviceIdType.MESH
LANES = 128
CORES = 2
WAYS = 2
UNITS = 3
SLOTS = UNITS * WAYS
BLOCK = CORES * WAYS * LANES
LONE = UNITS * WAYS - 1
STEPS = 127 * 256


def first_single(len_ref, n_seq):
    slot = jnp.int32(n_seq - 1)
    for s in reversed(range(n_seq - 1)):
        slot = jnp.where(len_ref[s] == 1, jnp.int32(s), slot)
    return slot


def split_sum(total, rows):
    high = total.astype(jnp.bfloat16)
    wide = high.astype(jnp.float32)
    left = jnp.round((total - wide) / jnp.where(wide == 0.0, 1.0, wide) * STEPS)
    low = left[:rows // 2] * 256.0 + left[rows // 2:]
    return high, low.astype(jnp.int32).astype(jnp.int16)


def join_sum(high, low):
    pair = low.astype(jnp.int32).astype(jnp.float32)
    first = jnp.round(pair * (1.0 / 256.0))
    left = jnp.concatenate([first, pair - first * 256.0], axis=0)
    wide = high.astype(jnp.float32)
    return wide + wide * (left * (1.0 / STEPS))


def split_lone(total):
    high = total.astype(jnp.bfloat16).astype(jnp.float32)
    return jnp.concatenate([high, total - high], axis=0).astype(jnp.bfloat16)


def join_lone(both):
    both = both.astype(jnp.float32)
    return both[:8] + both[8:]


class Rows:
    def __init__(self, tall, tail):
        self.tall, self.tail = tall, tail
        self.total = SLOTS * tall + tail

    def lone(self):
        return pl.ds(LONE * self.tall, self.tail)

    def tile(self, u, d):
        i = u * WAYS + d
        return pl.ds(i * self.tall + (self.tail if i >= LONE else 0), self.tall)

    def pair(self, u):
        return pl.ds(u * WAYS * self.tall, WAYS * self.tall + (self.tail if u == UNITS - 1 else 0))

    def half(self, u, d, lone=True):
        i = u * WAYS + d
        more = self.tail if (u == UNITS - 1 and lone) else 0
        start = i * self.tall + (self.tail if (i >= LONE and not lone) else 0)
        return pl.ds(start, self.tall + more)


def reduce_kernel(
    chips, n_seq, seq_len,
    len_ref, x_hbm, w_hbm, y_ref,
    x_raw, xc, wbuf, part, part_in, tx_hi, tx_lo, rx_hi, rx_lo, ag, ag_pair, keep, alone,
    x_sem, w_sem, pp_send, pp_recv, hi_send, hi_recv, lo_send, lo_recv, ag_send, ag_recv, ap_send, ap_recv,
):
    me = lax.axis_index("tp")
    z, core = me // CORES, lax.rem(me, CORES)
    nxt = lax.rem(z + 1, chips) * CORES + core
    prv = lax.rem(z + chips - 1, chips) * CORES + core
    mate = z * CORES + (1 - core)
    body_rows = (n_seq - 1) * seq_len
    far = chips // 2
    last = UNITS - 1
    wide, packed, low = Rows(body_rows, 8), Rows(body_rows, 16), Rows(body_rows // 2, 0)

    def place(t, side):
        return jnp.where(t == 0, 0, jnp.where(t == far, 2 * far - 1, 2 * t - 1 + side))

    def w_copy(t, u, side):
        chunk = lax.rem(z + chips + (t - far if side == 0 else far - t), chips)
        col = pl.multiple_of((chunk * UNITS + u) * BLOCK, BLOCK)
        b = u * WAYS + side
        return pltpu.make_async_copy(w_hbm.at[:, pl.ds(col, BLOCK)], wbuf.at[b], w_sem.at[b])

    x_copy = pltpu.make_async_copy(x_hbm, x_raw, x_sem)
    x_copy.start()
    w_copy(0, 0, 0).start()

    barrier = pltpu.get_barrier_semaphore()
    for peer in (mate, nxt, prv):
        pl.semaphore_signal(barrier, inc=1, device_id={"tp": peer}, device_id_type=MESH)

    single = first_single(len_ref, n_seq)
    x_copy.wait()
    w_copy(0, 1, 0).start()

    def x_rows(slot, count):
        return x_raw[slot * seq_len:slot * seq_len + count, :]

    for p in range(n_seq - 1):
        xc[p * seq_len:(p + 1) * seq_len, :] = jnp.where(single <= p, x_rows(p + 1, seq_len), x_rows(p, seq_len))
    lone = x_rows(n_seq - 1, 16)
    for s in range(n_seq - 1):
        lone = jnp.where(single == s, x_rows(s, 16), lone)
    xc[body_rows:body_rows + 16, :] = lone
    row = lax.broadcasted_iota(jnp.int32, (seq_len, LANES), 0)
    zero = jnp.bfloat16(0)
    for s in range(n_seq):
        many = jnp.where(single == s, 0, len_ref[s])
        one = jnp.where(single == s, 1, 0)
        keep[s * seq_len:(s + 1) * seq_len, :] = jnp.where(row < many, 1.0, 0.0).astype(jnp.bfloat16)
        alone[s * 16:(s + 1) * 16, :] = jnp.where(row[:16] < one, 1.0, 0.0).astype(jnp.bfloat16)
    pl.semaphore_wait(barrier, 3)

    def out_cols(slot, i, owner):
        chunk = lax.rem(z + chips - slot, chips)
        return pl.ds(pl.multiple_of(((chunk * SLOTS + i) * CORES + owner) * LANES, LANES), LANES)

    def expand(slot, u, ways, ref, owner):
        for d in ways:
            cols = out_cols(slot, u * WAYS + d, owner)
            top = packed.tile(u, d).start
            block = [ref[slot, top + p * seq_len:top + (p + 1) * seq_len, :] for p in range(n_seq - 1)]
            for s in range(n_seq):
                if s == 0 or s == n_seq - 1:
                    rows = block[min(s, n_seq - 2)]
                else:
                    rows = jnp.where(single < s, block[s - 1], block[s])
                mask = keep[s * seq_len:(s + 1) * seq_len, :]
                y_ref[s * seq_len:(s + 1) * seq_len, cols] = jnp.where(mask > zero, rows, zero)

    def expand_lone(slot, ref, owner):
        tail = ref[slot, packed.lone(), :].astype(jnp.float32)
        for i in range(SLOTS):
            cols = out_cols(slot, i, owner)
            value = jnp.broadcast_to(tail[i:i + 1, :], (16, LANES)).astype(jnp.bfloat16)
            for s in range(n_seq):
                rows = slice(s * seq_len, s * seq_len + 16)
                y_ref[rows, cols] = jnp.where(alone[s * 16:(s + 1) * 16, :] > zero, value, y_ref[rows, cols])

    def pp_copy(t, u, side):
        q = place(t, side)
        return pltpu.make_async_remote_copy(
            src_ref=part.at[1 - core, q, wide.pair(u)], dst_ref=part_in.at[q, wide.pair(u)],
            send_sem=pp_send.at[q, u], recv_sem=pp_recv.at[q, u], device_id={"tp": mate}, device_id_type=MESH)

    def rs_copies(t, u, side, far_end):
        peer = prv if side == 0 else nxt
        copies = []
        for tx, rx, ss, rs, rows in ((tx_hi, rx_hi, hi_send, hi_recv, packed), (tx_lo, rx_lo, lo_send, lo_recv, low)):
            where = rows.half(u, side) if far_end else rows.pair(u)
            copies.append(pltpu.make_async_remote_copy(
                src_ref=tx.at[side, t, where], dst_ref=rx.at[side, t, where],
                send_sem=ss.at[side, t, u], recv_sem=rs.at[side, t, u], device_id={"tp": peer}, device_id_type=MESH))
        return copies

    def ag_where(u, way, half):
        return packed.half(u, way, lone=way == 0) if half else packed.pair(u)

    def slot_of(h, way):
        return h if way == 0 else lax.rem(2 * far - h, 2 * far)

    def ag_copy(h, u, way, half):
        where = ag_where(u, way, half)
        return pltpu.make_async_remote_copy(
            src_ref=ag.at[slot_of(h, way), where], dst_ref=ag.at[slot_of(h + 1, way), where],
            send_sem=ag_send.at[way, h, u], recv_sem=ag_recv.at[way, h, u],
            device_id={"tp": nxt if way == 0 else prv}, device_id_type=MESH)

    def ap_copy(h, u, way, half=False):
        where = ag_where(u, way, half)
        return pltpu.make_async_remote_copy(
            src_ref=ag.at[slot_of(h, way), where], dst_ref=ag_pair.at[slot_of(h, way), where],
            send_sem=ap_send.at[way, h, u], recv_sem=ap_recv.at[way, h, u], device_id={"tp": mate}, device_id_type=MESH)

    def compute(t, u, side):
        q = place(t, side)
        w_copy(t, u, side).wait()
        if u == 0 and side == 0:
            @pl.when(t == 0)
            def _():
                for v in range(2, UNITS):
                    w_copy(0, v, 0).start()
                for v in range(UNITS):
                    w_copy(1, v, 1).start()

        prod = jnp.dot(xc[...], wbuf[u * WAYS + side], preferred_element_type=jnp.float32)
        for d in range(WAYS):
            i = u * WAYS + d
            for half in range(CORES):
                cols = slice((d * CORES + half) * LANES, (d * CORES + half + 1) * LANES)
                part[half, q, wide.tile(u, d), :] = prod[:body_rows, cols]
                tile = LONE * body_rows
                if i == 0:
                    part[half, q, tile:tile + 8, :] = prod[body_rows:body_rows + 8, cols]
                else:
                    part[half, q, tile + i:tile + i + 1, :] = prod[body_rows:body_rows + 1, cols]
        pp_copy(t, u, side).start()

        @pl.when(t < (far if side == 0 else far - 1))
        def _():
            w_copy(t + 1, u, side).start()

    def ring(t, u, side):
        q = place(t, side)
        parity = lax.rem(lax.broadcasted_iota(jnp.int32, (8, LANES), 0), WAYS)

        def here(where):
            return part[core, q, where, :] + part_in[q, where, :]

        def arrived(side_, d):
            return join_sum(rx_hi[side_, t - 1, packed.tile(u, d), :], rx_lo[side_, t - 1, low.tile(u, d), :])

        def arrived_lone(side_):
            return join_lone(rx_hi[side_, t - 1, packed.lone(), :])

        def put(side_, d, total):
            tx_hi[side_, t, packed.tile(u, d), :], tx_lo[side_, t, low.tile(u, d), :] = split_sum(total, body_rows)

        def put_lone(side_, total):
            tx_hi[side_, t, packed.lone(), :] = split_lone(total)

        if side == 0:
            @pl.when(t == 0)
            def _():
                pp_copy(t, u, side).wait_recv()
                for d in range(WAYS):
                    put(d, d, here(wide.tile(u, d)))
                    if u == last:
                        put_lone(d, here(wide.lone()))
                    for copy in rs_copies(0, u, d, True):
                        copy.start()

        @pl.when(t == 1)
        def _():
            pp_copy(t, u, side).wait_recv()
            put(side, 1 - side, here(wide.tile(u, 1 - side)))
            for copy in rs_copies(0, u, side, True):
                copy.wait_recv()
            put(side, side, here(wide.tile(u, side)) + arrived(side, side))
            if u == last:
                put_lone(side, here(wide.lone()) + jnp.where(parity == side, arrived_lone(side), 0.0))
            for copy in rs_copies(1, u, side, False):
                copy.start()

        @pl.when(jnp.logical_and(t > 1, t < far))
        def _():
            pp_copy(t, u, side).wait_recv()
            for copy in rs_copies(t - 1, u, side, False):
                copy.wait_recv()
            for d in range(WAYS):
                put(side, d, here(wide.tile(u, d)) + arrived(side, d))
            if u == last:
                put_lone(side, here(wide.lone()) + arrived_lone(side))
            for copy in rs_copies(t, u, side, False):
                copy.start()

        if side == 0:
            @pl.when(t == far)
            def _():
                pp_copy(t, u, side).wait_recv()
                for way in range(WAYS):
                    for copy in rs_copies(t - 1, u, way, False):
                        copy.wait_recv()
                for d in range(WAYS):
                    total = (here(wide.tile(u, d)) + arrived(0, d)) + arrived(1, d)
                    ag[0, packed.tile(u, d), :] = total.astype(jnp.bfloat16)
                if u == last:
                    total = (here(wide.lone()) + arrived_lone(0)) + arrived_lone(1)
                    ag[0, packed.lone(), :] = jnp.concatenate([total, total], axis=0).astype(jnp.bfloat16)
                for way in range(WAYS):
                    ag_copy(0, u, way, False).start()
                ap_copy(0, u, 0).start()
                expand(0, u, range(WAYS), ag, core)
                if u == last:
                    expand_lone(0, ag, core)

    turns = [(u, side) for u in range(UNITS) for side in range(WAYS)]

    @pl.loop(0, far + 1)
    def _(t):
        for i, (u, side) in enumerate(turns):
            if side == 0:
                compute(t, u, side)
            else:
                @pl.when(jnp.logical_and(t > 0, t < far))
                def _():
                    compute(t, u, side)
            if i >= 2:
                ring(t, *turns[i - 2])
            else:
                @pl.when(t > 0)
                def _():
                    ring(t - 1, *turns[i - 2])

    ring(jnp.int32(far), *turns[-2])

    def mates(h, u, way):
        ap_copy(h, u, way).wait_recv()
        expand(slot_of(h, way), u, range(WAYS), ag_pair, 1 - core)
        if u == last:
            expand_lone(slot_of(h, way), ag_pair, 1 - core)

    for h in range(1, far):
        for u in range(UNITS):
            for way in range(WAYS):
                ag_copy(h - 1, u, way, False).wait_recv()
                ag_copy(h, u, way, h == far - 1).start()
                ap_copy(h, u, way).start()
                expand(slot_of(h, way), u, range(WAYS), ag, core)
                if u == last:
                    expand_lone(slot_of(h, way), ag, core)
                if h > 1 or way == 0:
                    mates(h - 1, u, way)
    for u in range(UNITS):
        for way in range(WAYS):
            ag_copy(far - 1, u, way, True).wait_recv()
            ap_copy(far, u, way, True).start()
            expand(far, u, (way,), ag, core)
            mates(far - 1, u, way)
    expand_lone(far, ag, core)
    for u in range(UNITS):
        for way in range(WAYS):
            ap_copy(far, u, way, True).wait_recv()
            expand(far, u, (way,), ag_pair, 1 - core)
    expand_lone(far, ag_pair, 1 - core)

    for u in range(UNITS):
        ap_copy(0, u, 0).wait_send()
        for side in range(WAYS):
            for copy in rs_copies(0, u, side, True):
                copy.wait_send()
            ag_copy(far - 1, u, side, True).wait_send()
            ap_copy(far, u, side, True).wait_send()

    @pl.loop(0, 2 * far)
    def _(q):
        for u in range(UNITS):
            pltpu.make_async_remote_copy(
                src_ref=part.at[1 - core, q, wide.pair(u)], dst_ref=part_in.at[q, wide.pair(u)],
                send_sem=pp_send.at[q, u], recv_sem=pp_recv.at[q, u], device_id={"tp": mate}, device_id_type=MESH).wait_send()

    @pl.loop(1, far)
    def _(t):
        for u in range(UNITS):
            for side in range(WAYS):
                for copy in rs_copies(t, u, side, False):
                    copy.wait_send()
                ag_copy(t - 1, u, side, False).wait_send()
                ap_copy(t, u, side).wait_send()


def solution(mesh):
    chips = mesh.shape["tp"] // CORES

    def local_part(x_loc, w_loc, lengths):
        tokens, depth = x_loc.shape
        columns = w_loc.shape[1]
        n_seq = lengths.shape[0]
        seq_len = tokens // n_seq
        body_rows = (n_seq - 1) * seq_len
        far = chips // 2
        assert columns == chips * UNITS * BLOCK and chips == 2 * far and far >= 3
        wide, packed, low = Rows(body_rows, 8), Rows(body_rows, 16), Rows(body_rows // 2, 0)
        dma = pltpu.SemaphoreType.DMA
        held = pltpu.VMEM((chips, packed.total, LANES), jnp.bfloat16)
        vmem = pl.BlockSpec(memory_space=pltpu.VMEM)
        smem = pl.BlockSpec(memory_space=pltpu.SMEM)
        hbm = pl.BlockSpec(memory_space=pl.ANY)
        high = pltpu.VMEM((WAYS, far, packed.total, LANES), jnp.bfloat16)
        lows = pltpu.VMEM((WAYS, far, low.total, LANES), jnp.int16)
        hops = dma((WAYS, far, UNITS))
        return pl.pallas_call(
            functools.partial(reduce_kernel, chips, n_seq, seq_len),
            out_shape=pltpu.VMEM((tokens, columns), jnp.bfloat16),
            in_specs=[smem, hbm, hbm],
            out_specs=vmem,
            scratch_shapes=[
                pltpu.VMEM((tokens, depth), jnp.bfloat16),
                pltpu.VMEM((body_rows + 16, depth), jnp.bfloat16),
                pltpu.VMEM((SLOTS, depth, BLOCK), jnp.bfloat16),
                pltpu.VMEM((CORES, chips, wide.total, LANES), jnp.float32),
                pltpu.VMEM((chips, wide.total, LANES), jnp.float32),
                high, lows, high, lows, held, held,
                pltpu.VMEM((tokens, LANES), jnp.bfloat16),
                pltpu.VMEM((n_seq * 16, LANES), jnp.bfloat16),
                dma,
                dma((SLOTS,)),
                dma((chips, UNITS)), dma((chips, UNITS)),
                hops, hops, hops, hops, hops, hops,
                dma((WAYS, far + 1, UNITS)), dma((WAYS, far + 1, UNITS)),
            ],
            compiler_params=pltpu.CompilerParams(
                collective_id=0, has_side_effects=True, vmem_limit_bytes=54 * 1024 * 1024),
            name="reduce_gather",
        )(lengths, x_loc, w_loc)

    return jax.shard_map(local_part, mesh=mesh, in_specs=(P("data", "tp"), P("tp", None), P("data")), out_specs=P("data", None), check_vma=False)
```

```python
import functools

import jax
import jax.numpy as jnp
from jax import lax
from jax.experimental import pallas as pl
from jax.experimental.pallas import tpu as pltpu
from jax.sharding import PartitionSpec as P

MESH = pl.DeviceIdType.MESH
LANES = 128
CORES = 2
WAYS = 2
UNITS = 3
SLOTS = UNITS * WAYS
BLOCK = CORES * WAYS * LANES
LONE = UNITS * WAYS - 1
LOWS = 3
LEVELS = 39
STEPS = (LEVELS // 2) * 256


def first_single(len_ref, n_seq):
    slot = jnp.int32(n_seq - 1)
    for s in reversed(range(n_seq - 1)):
        slot = jnp.where(len_ref[s] == 1, jnp.int32(s), slot)
    return slot


def split_sum(total, rows):
    high = total.astype(jnp.bfloat16)
    wide = high.astype(jnp.float32)
    left = jnp.round((total - wide) / jnp.where(wide == 0.0, 1.0, wide) * STEPS)
    third = rows // LOWS
    low = (left[:third] * LEVELS + left[third:2 * third]) * LEVELS + left[2 * third:]
    return high, low.astype(jnp.int32).astype(jnp.int16)


def join_sum(high, low):
    code = low.astype(jnp.int32).astype(jnp.float32)
    first = jnp.round(code * (1.0 / LEVELS ** 2))
    rest = code - first * LEVELS ** 2
    second = jnp.round(rest * (1.0 / LEVELS))
    left = jnp.concatenate([first, second, rest - second * LEVELS], axis=0)
    wide = high.astype(jnp.float32)
    return wide + wide * (left * (1.0 / STEPS))


def split_lone(total):
    high = total.astype(jnp.bfloat16).astype(jnp.float32)
    return jnp.concatenate([high, total - high], axis=0).astype(jnp.bfloat16)


def join_lone(both):
    both = both.astype(jnp.float32)
    return both[:8] + both[8:]


class Rows:
    def __init__(self, tall, tail):
        self.tall, self.tail = tall, tail
        self.total = SLOTS * tall + tail

    def lone(self):
        return pl.ds(LONE * self.tall, self.tail)

    def tile(self, u, d):
        i = u * WAYS + d
        return pl.ds(i * self.tall + (self.tail if i >= LONE else 0), self.tall)

    def pair(self, u):
        return pl.ds(u * WAYS * self.tall, WAYS * self.tall + (self.tail if u == UNITS - 1 else 0))

    def half(self, u, d, lone=True):
        i = u * WAYS + d
        more = self.tail if (u == UNITS - 1 and lone) else 0
        start = i * self.tall + (self.tail if (i >= LONE and not lone) else 0)
        return pl.ds(start, self.tall + more)


def reduce_kernel(
    chips, n_seq, seq_len,
    len_ref, x_hbm, w_hbm, y_ref,
    x_raw, xc, wbuf, part, part_in, tx_hi, tx_lo, rx_hi, rx_lo, ag, ag_pair, keep, alone,
    x_sem, w_sem, pp_send, pp_recv, hi_send, hi_recv, lo_send, lo_recv, ag_send, ag_recv, ap_send, ap_recv,
):
    me = lax.axis_index("tp")
    z, core = me // CORES, lax.rem(me, CORES)
    nxt = lax.rem(z + 1, chips) * CORES + core
    prv = lax.rem(z + chips - 1, chips) * CORES + core
    mate = z * CORES + (1 - core)
    body_rows = (n_seq - 1) * seq_len
    far = chips // 2
    last = UNITS - 1
    wide, packed, low = Rows(body_rows, 8), Rows(body_rows, 16), Rows(body_rows // LOWS, 0)

    def place(t, side):
        return jnp.where(t == 0, 0, jnp.where(t == far, 2 * far - 1, 2 * t - 1 + side))

    def w_copy(t, u, side):
        chunk = lax.rem(z + chips + (t - far if side == 0 else far - t), chips)
        col = pl.multiple_of((chunk * UNITS + u) * BLOCK, BLOCK)
        b = u * WAYS + side
        return pltpu.make_async_copy(w_hbm.at[:, pl.ds(col, BLOCK)], wbuf.at[b], w_sem.at[b])

    x_copy = pltpu.make_async_copy(x_hbm, x_raw, x_sem)
    x_copy.start()
    w_copy(0, 0, 0).start()

    barrier = pltpu.get_barrier_semaphore()
    for peer in (mate, nxt, prv):
        pl.semaphore_signal(barrier, inc=1, device_id={"tp": peer}, device_id_type=MESH)

    single = first_single(len_ref, n_seq)
    x_copy.wait()
    w_copy(0, 1, 0).start()

    def x_rows(slot, count):
        return x_raw[slot * seq_len:slot * seq_len + count, :]

    for p in range(n_seq - 1):
        xc[p * seq_len:(p + 1) * seq_len, :] = jnp.where(single <= p, x_rows(p + 1, seq_len), x_rows(p, seq_len))
    lone = x_rows(n_seq - 1, 16)
    for s in range(n_seq - 1):
        lone = jnp.where(single == s, x_rows(s, 16), lone)
    xc[body_rows:body_rows + 16, :] = lone
    row = lax.broadcasted_iota(jnp.int32, (seq_len, LANES), 0)
    zero = jnp.bfloat16(0)
    for s in range(n_seq):
        many = jnp.where(single == s, 0, len_ref[s])
        one = jnp.where(single == s, 1, 0)
        keep[s * seq_len:(s + 1) * seq_len, :] = jnp.where(row < many, 1.0, 0.0).astype(jnp.bfloat16)
        alone[s * 16:(s + 1) * 16, :] = jnp.where(row[:16] < one, 1.0, 0.0).astype(jnp.bfloat16)
    pl.semaphore_wait(barrier, 3)

    def out_cols(slot, i, owner):
        chunk = lax.rem(z + chips - slot, chips)
        return pl.ds(pl.multiple_of(((chunk * SLOTS + i) * CORES + owner) * LANES, LANES), LANES)

    def expand(slot, u, ways, ref, owner):
        for d in ways:
            cols = out_cols(slot, u * WAYS + d, owner)
            top = packed.tile(u, d).start
            block = [ref[slot, top + p * seq_len:top + (p + 1) * seq_len, :] for p in range(n_seq - 1)]
            for s in range(n_seq):
                if s == 0 or s == n_seq - 1:
                    rows = block[min(s, n_seq - 2)]
                else:
                    rows = jnp.where(single < s, block[s - 1], block[s])
                mask = keep[s * seq_len:(s + 1) * seq_len, :]
                y_ref[s * seq_len:(s + 1) * seq_len, cols] = jnp.where(mask > zero, rows, zero)

    def expand_lone(slot, ref, owner):
        tail = ref[slot, packed.lone(), :].astype(jnp.float32)
        for i in range(SLOTS):
            cols = out_cols(slot, i, owner)
            value = jnp.broadcast_to(tail[i:i + 1, :], (16, LANES)).astype(jnp.bfloat16)
            for s in range(n_seq):
                rows = slice(s * seq_len, s * seq_len + 16)
                y_ref[rows, cols] = jnp.where(alone[s * 16:(s + 1) * 16, :] > zero, value, y_ref[rows, cols])

    def pp_copy(t, u, side):
        q = place(t, side)
        return pltpu.make_async_remote_copy(
            src_ref=part.at[1 - core, q, wide.pair(u)], dst_ref=part_in.at[q, wide.pair(u)],
            send_sem=pp_send.at[q, u], recv_sem=pp_recv.at[q, u], device_id={"tp": mate}, device_id_type=MESH)

    def rs_copies(t, u, side, far_end):
        peer = prv if side == 0 else nxt
        copies = []
        for tx, rx, ss, rs, rows in ((tx_hi, rx_hi, hi_send, hi_recv, packed), (tx_lo, rx_lo, lo_send, lo_recv, low)):
            where = rows.half(u, side) if far_end else rows.pair(u)
            copies.append(pltpu.make_async_remote_copy(
                src_ref=tx.at[side, t, where], dst_ref=rx.at[side, t, where],
                send_sem=ss.at[side, t, u], recv_sem=rs.at[side, t, u], device_id={"tp": peer}, device_id_type=MESH))
        return copies

    def ag_where(u, way, half):
        return packed.half(u, way, lone=way == 0) if half else packed.pair(u)

    def slot_of(h, way):
        return h if way == 0 else lax.rem(2 * far - h, 2 * far)

    def ag_copy(h, u, way, half):
        where = ag_where(u, way, half)
        return pltpu.make_async_remote_copy(
            src_ref=ag.at[slot_of(h, way), where], dst_ref=ag.at[slot_of(h + 1, way), where],
            send_sem=ag_send.at[way, h, u], recv_sem=ag_recv.at[way, h, u],
            device_id={"tp": nxt if way == 0 else prv}, device_id_type=MESH)

    def ap_copy(h, u, way, half=False):
        where = ag_where(u, way, half)
        return pltpu.make_async_remote_copy(
            src_ref=ag.at[slot_of(h, way), where], dst_ref=ag_pair.at[slot_of(h, way), where],
            send_sem=ap_send.at[way, h, u], recv_sem=ap_recv.at[way, h, u], device_id={"tp": mate}, device_id_type=MESH)

    def compute(t, u, side):
        q = place(t, side)
        w_copy(t, u, side).wait()
        if u == 0 and side == 0:
            @pl.when(t == 0)
            def _():
                for v in range(2, UNITS):
                    w_copy(0, v, 0).start()
                for v in range(UNITS):
                    w_copy(1, v, 1).start()

        prod = jnp.dot(xc[...], wbuf[u * WAYS + side], preferred_element_type=jnp.float32)
        for d in range(WAYS):
            i = u * WAYS + d
            for half in range(CORES):
                cols = slice((d * CORES + half) * LANES, (d * CORES + half + 1) * LANES)
                part[half, q, wide.tile(u, d), :] = prod[:body_rows, cols]
                tile = LONE * body_rows
                if i == 0:
                    part[half, q, tile:tile + 8, :] = prod[body_rows:body_rows + 8, cols]
                else:
                    part[half, q, tile + i:tile + i + 1, :] = prod[body_rows:body_rows + 1, cols]
        pp_copy(t, u, side).start()

        @pl.when(t < (far if side == 0 else far - 1))
        def _():
            w_copy(t + 1, u, side).start()

    def ring(t, u, side):
        q = place(t, side)
        parity = lax.rem(lax.broadcasted_iota(jnp.int32, (8, LANES), 0), WAYS)

        def here(where):
            return part[core, q, where, :] + part_in[q, where, :]

        def arrived(side_, d):
            return join_sum(rx_hi[side_, t - 1, packed.tile(u, d), :], rx_lo[side_, t - 1, low.tile(u, d), :])

        def arrived_lone(side_):
            return join_lone(rx_hi[side_, t - 1, packed.lone(), :])

        def put(side_, d, total):
            tx_hi[side_, t, packed.tile(u, d), :], tx_lo[side_, t, low.tile(u, d), :] = split_sum(total, body_rows)

        def put_lone(side_, total):
            tx_hi[side_, t, packed.lone(), :] = split_lone(total)

        if side == 0:
            @pl.when(t == 0)
            def _():
                pp_copy(t, u, side).wait_recv()
                for d in range(WAYS):
                    put(d, d, here(wide.tile(u, d)))
                    if u == last:
                        put_lone(d, here(wide.lone()))
                    for copy in rs_copies(0, u, d, True):
                        copy.start()

        @pl.when(t == 1)
        def _():
            pp_copy(t, u, side).wait_recv()
            put(side, 1 - side, here(wide.tile(u, 1 - side)))
            for copy in rs_copies(0, u, side, True):
                copy.wait_recv()
            put(side, side, here(wide.tile(u, side)) + arrived(side, side))
            if u == last:
                put_lone(side, here(wide.lone()) + jnp.where(parity == side, arrived_lone(side), 0.0))
            for copy in rs_copies(1, u, side, False):
                copy.start()

        @pl.when(jnp.logical_and(t > 1, t < far))
        def _():
            pp_copy(t, u, side).wait_recv()
            for copy in rs_copies(t - 1, u, side, False):
                copy.wait_recv()
            for d in range(WAYS):
                put(side, d, here(wide.tile(u, d)) + arrived(side, d))
            if u == last:
                put_lone(side, here(wide.lone()) + arrived_lone(side))
            for copy in rs_copies(t, u, side, False):
                copy.start()

        if side == 0:
            @pl.when(t == far)
            def _():
                pp_copy(t, u, side).wait_recv()
                for way in range(WAYS):
                    for copy in rs_copies(t - 1, u, way, False):
                        copy.wait_recv()
                for d in range(WAYS):
                    total = (here(wide.tile(u, d)) + arrived(0, d)) + arrived(1, d)
                    ag[0, packed.tile(u, d), :] = total.astype(jnp.bfloat16)
                if u == last:
                    total = (here(wide.lone()) + arrived_lone(0)) + arrived_lone(1)
                    ag[0, packed.lone(), :] = jnp.concatenate([total, total], axis=0).astype(jnp.bfloat16)
                for way in range(WAYS):
                    ag_copy(0, u, way, False).start()
                ap_copy(0, u, 0).start()
                expand(0, u, range(WAYS), ag, core)
                if u == last:
                    expand_lone(0, ag, core)

    turns = [(u, side) for u in range(UNITS) for side in range(WAYS)]

    @pl.loop(0, far + 1)
    def _(t):
        for i, (u, side) in enumerate(turns):
            if side == 0:
                compute(t, u, side)
            else:
                @pl.when(jnp.logical_and(t > 0, t < far))
                def _():
                    compute(t, u, side)
            if i >= 2:
                ring(t, *turns[i - 2])
            else:
                @pl.when(t > 0)
                def _():
                    ring(t - 1, *turns[i - 2])

    ring(jnp.int32(far), *turns[-2])

    def mates(h, u, way):
        ap_copy(h, u, way).wait_recv()
        expand(slot_of(h, way), u, range(WAYS), ag_pair, 1 - core)
        if u == last:
            expand_lone(slot_of(h, way), ag_pair, 1 - core)

    for h in range(1, far):
        for u in range(UNITS):
            for way in range(WAYS):
                ag_copy(h - 1, u, way, False).wait_recv()
                ag_copy(h, u, way, h == far - 1).start()
                ap_copy(h, u, way).start()
                expand(slot_of(h, way), u, range(WAYS), ag, core)
                if u == last:
                    expand_lone(slot_of(h, way), ag, core)
                if h > 1 or way == 0:
                    mates(h - 1, u, way)
    for u in range(UNITS):
        for way in range(WAYS):
            ag_copy(far - 1, u, way, True).wait_recv()
            ap_copy(far, u, way, True).start()
            expand(far, u, (way,), ag, core)
            mates(far - 1, u, way)
    expand_lone(far, ag, core)
    for u in range(UNITS):
        for way in range(WAYS):
            ap_copy(far, u, way, True).wait_recv()
            expand(far, u, (way,), ag_pair, 1 - core)
    expand_lone(far, ag_pair, 1 - core)

    for u in range(UNITS):
        ap_copy(0, u, 0).wait_send()
        for side in range(WAYS):
            for copy in rs_copies(0, u, side, True):
                copy.wait_send()
            ag_copy(far - 1, u, side, True).wait_send()
            ap_copy(far, u, side, True).wait_send()

    @pl.loop(0, 2 * far)
    def _(q):
        for u in range(UNITS):
            pltpu.make_async_remote_copy(
                src_ref=part.at[1 - core, q, wide.pair(u)], dst_ref=part_in.at[q, wide.pair(u)],
                send_sem=pp_send.at[q, u], recv_sem=pp_recv.at[q, u], device_id={"tp": mate}, device_id_type=MESH).wait_send()

    @pl.loop(1, far)
    def _(t):
        for u in range(UNITS):
            for side in range(WAYS):
                for copy in rs_copies(t, u, side, False):
                    copy.wait_send()
                ag_copy(t - 1, u, side, False).wait_send()
                ap_copy(t, u, side).wait_send()


def solution(mesh):
    chips = mesh.shape["tp"] // CORES

    def local_part(x_loc, w_loc, lengths):
        tokens, depth = x_loc.shape
        columns = w_loc.shape[1]
        n_seq = lengths.shape[0]
        seq_len = tokens // n_seq
        body_rows = (n_seq - 1) * seq_len
        far = chips // 2
        assert columns == chips * UNITS * BLOCK and chips == 2 * far and far >= 3
        wide, packed, low = Rows(body_rows, 8), Rows(body_rows, 16), Rows(body_rows // LOWS, 0)
        dma = pltpu.SemaphoreType.DMA
        held = pltpu.VMEM((chips, packed.total, LANES), jnp.bfloat16)
        vmem = pl.BlockSpec(memory_space=pltpu.VMEM)
        smem = pl.BlockSpec(memory_space=pltpu.SMEM)
        hbm = pl.BlockSpec(memory_space=pl.ANY)
        high = pltpu.VMEM((WAYS, far, packed.total, LANES), jnp.bfloat16)
        lows = pltpu.VMEM((WAYS, far, low.total, LANES), jnp.int16)
        hops = dma((WAYS, far, UNITS))
        return pl.pallas_call(
            functools.partial(reduce_kernel, chips, n_seq, seq_len),
            out_shape=pltpu.VMEM((tokens, columns), jnp.bfloat16),
            in_specs=[smem, hbm, hbm],
            out_specs=vmem,
            scratch_shapes=[
                pltpu.VMEM((tokens, depth), jnp.bfloat16),
                pltpu.VMEM((body_rows + 16, depth), jnp.bfloat16),
                pltpu.VMEM((SLOTS, depth, BLOCK), jnp.bfloat16),
                pltpu.VMEM((CORES, chips, wide.total, LANES), jnp.float32),
                pltpu.VMEM((chips, wide.total, LANES), jnp.float32),
                high, lows, high, lows, held, held,
                pltpu.VMEM((tokens, LANES), jnp.bfloat16),
                pltpu.VMEM((n_seq * 16, LANES), jnp.bfloat16),
                dma,
                dma((SLOTS,)),
                dma((chips, UNITS)), dma((chips, UNITS)),
                hops, hops, hops, hops, hops, hops,
                dma((WAYS, far + 1, UNITS)), dma((WAYS, far + 1, UNITS)),
            ],
            compiler_params=pltpu.CompilerParams(
                collective_id=0, has_side_effects=True, vmem_limit_bytes=54 * 1024 * 1024),
            name="reduce_gather",
        )(lengths, x_loc, w_loc)

    return jax.shard_map(local_part, mesh=mesh, in_specs=(P("data", "tp"), P("tp", None), P("data")), out_specs=P("data", None), check_vma=False)
```

```python
import functools

import jax
import jax.numpy as jnp
from jax import lax
from jax.experimental import pallas as pl
from jax.experimental.pallas import tpu as pltpu
from jax.sharding import PartitionSpec as P

MESH = pl.DeviceIdType.MESH
LANES = 128
CORES = 2
WAYS = 2
UNITS = 3
SLOTS = UNITS * WAYS
AHEAD = 3
BLOCK = CORES * WAYS * LANES
LONE = UNITS * WAYS - 1
LOWS = 3
LEVELS = 39
STEPS = (LEVELS // 2) * 256


def first_single(len_ref, n_seq):
    slot = jnp.int32(n_seq - 1)
    for s in reversed(range(n_seq - 1)):
        slot = jnp.where(len_ref[s] == 1, jnp.int32(s), slot)
    return slot


def split_sum(total, rows):
    high = total.astype(jnp.bfloat16)
    wide = high.astype(jnp.float32)
    left = jnp.round((total - wide) / jnp.where(wide == 0.0, 1.0, wide) * STEPS)
    third = rows // LOWS
    low = (left[:third] * LEVELS + left[third:2 * third]) * LEVELS + left[2 * third:]
    return high, low.astype(jnp.int32).astype(jnp.int16)


def join_sum(high, low):
    code = low.astype(jnp.int32).astype(jnp.float32)
    first = jnp.round(code * (1.0 / LEVELS ** 2))
    rest = code - first * LEVELS ** 2
    second = jnp.round(rest * (1.0 / LEVELS))
    left = jnp.concatenate([first, second, rest - second * LEVELS], axis=0)
    wide = high.astype(jnp.float32)
    return wide + wide * (left * (1.0 / STEPS))


def split_lone(total):
    high = total.astype(jnp.bfloat16).astype(jnp.float32)
    return jnp.concatenate([high, total - high], axis=0).astype(jnp.bfloat16)


def join_lone(both):
    both = both.astype(jnp.float32)
    return both[:8] + both[8:]


class Rows:
    def __init__(self, tall, tail):
        self.tall, self.tail = tall, tail
        self.total = SLOTS * tall + tail

    def lone(self):
        return pl.ds(LONE * self.tall, self.tail)

    def tile(self, u, d):
        i = u * WAYS + d
        return pl.ds(i * self.tall + (self.tail if i >= LONE else 0), self.tall)

    def pair(self, u):
        return pl.ds(u * WAYS * self.tall, WAYS * self.tall + (self.tail if u == UNITS - 1 else 0))

    def half(self, u, d, lone=True):
        i = u * WAYS + d
        more = self.tail if (u == UNITS - 1 and lone) else 0
        start = i * self.tall + (self.tail if (i >= LONE and not lone) else 0)
        return pl.ds(start, self.tall + more)


def reduce_kernel(
    chips, n_seq, seq_len,
    len_ref, x_hbm, w_hbm, y_ref,
    x_raw, xc, wbuf, part, part_in, tx_hi, tx_lo, rx_hi, rx_lo, ag, ag_pair, keep, alone,
    x_sem, w_sem, pp_send, pp_recv, hi_send, hi_recv, lo_send, lo_recv, ag_send, ag_recv, ap_send, ap_recv,
):
    me = lax.axis_index("tp")
    z, core = me // CORES, lax.rem(me, CORES)
    nxt = lax.rem(z + 1, chips) * CORES + core
    prv = lax.rem(z + chips - 1, chips) * CORES + core
    mate = z * CORES + (1 - core)
    body_rows = (n_seq - 1) * seq_len
    far = chips // 2
    last = UNITS - 1
    wide, packed, low = Rows(body_rows, 8), Rows(body_rows, 16), Rows(body_rows // LOWS, 0)

    def place(t, side):
        return jnp.where(t == 0, 0, jnp.where(t == far, 2 * far - 1, 2 * t - 1 + side))

    blocks = chips * UNITS

    def turn(t, u, side):
        middle = UNITS + (t - 1) * SLOTS + u * WAYS + side
        return jnp.where(t == 0, u, jnp.where(t == far, blocks - UNITS + u, middle))

    def w_copy(n):
        ends = jnp.where(n < UNITS, n, n - (blocks - UNITS))
        inner = jnp.logical_and(n >= UNITS, n < blocks - UNITS)
        i = jnp.where(inner, lax.rem(n + (SLOTS - UNITS), SLOTS), ends * WAYS)
        t = jnp.where(n < UNITS, 0, (n + (SLOTS - UNITS)) // SLOTS)
        u, side = i // WAYS, lax.rem(i, WAYS)
        chunk = lax.rem(z + chips + jnp.where(side == 0, t - far, far - t), chips)
        col = pl.multiple_of((chunk * UNITS + u) * BLOCK, BLOCK)
        b = lax.rem(n, SLOTS)
        return pltpu.make_async_copy(w_hbm.at[:, pl.ds(col, BLOCK)], wbuf.at[b], w_sem.at[b])

    x_copy = pltpu.make_async_copy(x_hbm, x_raw, x_sem)
    x_copy.start()
    w_copy(jnp.int32(0)).start()

    barrier = pltpu.get_barrier_semaphore()
    for peer in (mate, nxt, prv):
        pl.semaphore_signal(barrier, inc=1, device_id={"tp": peer}, device_id_type=MESH)

    single = first_single(len_ref, n_seq)
    x_copy.wait()
    w_copy(jnp.int32(1)).start()

    def x_rows(slot, count):
        return x_raw[slot * seq_len:slot * seq_len + count, :]

    for p in range(n_seq - 1):
        xc[p * seq_len:(p + 1) * seq_len, :] = jnp.where(single <= p, x_rows(p + 1, seq_len), x_rows(p, seq_len))
    lone = x_rows(n_seq - 1, 16)
    for s in range(n_seq - 1):
        lone = jnp.where(single == s, x_rows(s, 16), lone)
    xc[body_rows:body_rows + 16, :] = lone
    row = lax.broadcasted_iota(jnp.int32, (seq_len, LANES), 0)
    zero = jnp.bfloat16(0)
    for s in range(n_seq):
        many = jnp.where(single == s, 0, len_ref[s])
        one = jnp.where(single == s, 1, 0)
        keep[s * seq_len:(s + 1) * seq_len, :] = jnp.where(row < many, 1.0, 0.0).astype(jnp.bfloat16)
        alone[s * 16:(s + 1) * 16, :] = jnp.where(row[:16] < one, 1.0, 0.0).astype(jnp.bfloat16)
    pl.semaphore_wait(barrier, 3)

    def out_cols(slot, i, owner):
        chunk = lax.rem(z + chips - slot, chips)
        return pl.ds(pl.multiple_of(((chunk * SLOTS + i) * CORES + owner) * LANES, LANES), LANES)

    def expand(slot, u, ways, ref, owner):
        for d in ways:
            cols = out_cols(slot, u * WAYS + d, owner)
            top = packed.tile(u, d).start
            block = [ref[slot, top + p * seq_len:top + (p + 1) * seq_len, :] for p in range(n_seq - 1)]
            for s in range(n_seq):
                if s == 0 or s == n_seq - 1:
                    rows = block[min(s, n_seq - 2)]
                else:
                    rows = jnp.where(single < s, block[s - 1], block[s])
                mask = keep[s * seq_len:(s + 1) * seq_len, :]
                y_ref[s * seq_len:(s + 1) * seq_len, cols] = jnp.where(mask > zero, rows, zero)

    def expand_lone(slot, ref, owner):
        tail = ref[slot, packed.lone(), :].astype(jnp.float32)
        for i in range(SLOTS):
            cols = out_cols(slot, i, owner)
            value = jnp.broadcast_to(tail[i:i + 1, :], (16, LANES)).astype(jnp.bfloat16)
            for s in range(n_seq):
                rows = slice(s * seq_len, s * seq_len + 16)
                y_ref[rows, cols] = jnp.where(alone[s * 16:(s + 1) * 16, :] > zero, value, y_ref[rows, cols])

    def pp_copy(t, u, side):
        q = place(t, side)
        return pltpu.make_async_remote_copy(
            src_ref=part.at[1 - core, q, wide.pair(u)], dst_ref=part_in.at[q, wide.pair(u)],
            send_sem=pp_send.at[q, u], recv_sem=pp_recv.at[q, u], device_id={"tp": mate}, device_id_type=MESH)

    def rs_copies(t, u, side, far_end):
        peer = prv if side == 0 else nxt
        copies = []
        for tx, rx, ss, rs, rows in ((tx_hi, rx_hi, hi_send, hi_recv, packed), (tx_lo, rx_lo, lo_send, lo_recv, low)):
            where = rows.half(u, side) if far_end else rows.pair(u)
            copies.append(pltpu.make_async_remote_copy(
                src_ref=tx.at[side, t, where], dst_ref=rx.at[side, t, where],
                send_sem=ss.at[side, t, u], recv_sem=rs.at[side, t, u], device_id={"tp": peer}, device_id_type=MESH))
        return copies

    def ag_where(u, way, half):
        return packed.half(u, way, lone=way == 0) if half else packed.pair(u)

    def slot_of(h, way):
        return h if way == 0 else lax.rem(2 * far - h, 2 * far)

    def ag_copy(h, u, way, half):
        where = ag_where(u, way, half)
        return pltpu.make_async_remote_copy(
            src_ref=ag.at[slot_of(h, way), where], dst_ref=ag.at[slot_of(h + 1, way), where],
            send_sem=ag_send.at[way, h, u], recv_sem=ag_recv.at[way, h, u],
            device_id={"tp": nxt if way == 0 else prv}, device_id_type=MESH)

    def ap_copy(h, u, way, half=False):
        where = ag_where(u, way, half)
        return pltpu.make_async_remote_copy(
            src_ref=ag.at[slot_of(h, way), where], dst_ref=ag_pair.at[slot_of(h, way), where],
            send_sem=ap_send.at[way, h, u], recv_sem=ap_recv.at[way, h, u], device_id={"tp": mate}, device_id_type=MESH)

    def compute(t, u, side):
        q = place(t, side)
        n = turn(t, u, side)
        w_copy(n).wait()
        if u == 0 and side == 0:
            @pl.when(t == 0)
            def _():
                for early in range(2, AHEAD):
                    w_copy(jnp.int32(early)).start()

        @pl.when(n + AHEAD < blocks)
        def _():
            w_copy(n + AHEAD).start()

        prod = jnp.dot(xc[...], wbuf[lax.rem(n, SLOTS)], preferred_element_type=jnp.float32)
        for d in range(WAYS):
            i = u * WAYS + d
            for half in range(CORES):
                cols = slice((d * CORES + half) * LANES, (d * CORES + half + 1) * LANES)
                part[half, q, wide.tile(u, d), :] = prod[:body_rows, cols]
                tile = LONE * body_rows
                if i == 0:
                    part[half, q, tile:tile + 8, :] = prod[body_rows:body_rows + 8, cols]
                else:
                    part[half, q, tile + i:tile + i + 1, :] = prod[body_rows:body_rows + 1, cols]
        pp_copy(t, u, side).start()

    def ring(t, u, side):
        q = place(t, side)
        parity = lax.rem(lax.broadcasted_iota(jnp.int32, (8, LANES), 0), WAYS)

        def here(where):
            return part[core, q, where, :] + part_in[q, where, :]

        def arrived(side_, d):
            return join_sum(rx_hi[side_, t - 1, packed.tile(u, d), :], rx_lo[side_, t - 1, low.tile(u, d), :])

        def arrived_lone(side_):
            return join_lone(rx_hi[side_, t - 1, packed.lone(), :])

        def put(side_, d, total):
            tx_hi[side_, t, packed.tile(u, d), :], tx_lo[side_, t, low.tile(u, d), :] = split_sum(total, body_rows)

        def put_lone(side_, total):
            tx_hi[side_, t, packed.lone(), :] = split_lone(total)

        if side == 0:
            @pl.when(t == 0)
            def _():
                pp_copy(t, u, side).wait_recv()
                for d in range(WAYS):
                    put(d, d, here(wide.tile(u, d)))
                    if u == last:
                        put_lone(d, here(wide.lone()))
                    for copy in rs_copies(0, u, d, True):
                        copy.start()

        @pl.when(t == 1)
        def _():
            pp_copy(t, u, side).wait_recv()
            put(side, 1 - side, here(wide.tile(u, 1 - side)))
            for copy in rs_copies(0, u, side, True):
                copy.wait_recv()
            put(side, side, here(wide.tile(u, side)) + arrived(side, side))
            if u == last:
                put_lone(side, here(wide.lone()) + jnp.where(parity == side, arrived_lone(side), 0.0))
            for copy in rs_copies(1, u, side, False):
                copy.start()

        @pl.when(jnp.logical_and(t > 1, t < far))
        def _():
            pp_copy(t, u, side).wait_recv()
            for copy in rs_copies(t - 1, u, side, False):
                copy.wait_recv()
            for d in range(WAYS):
                put(side, d, here(wide.tile(u, d)) + arrived(side, d))
            if u == last:
                put_lone(side, here(wide.lone()) + arrived_lone(side))
            for copy in rs_copies(t, u, side, False):
                copy.start()

        if side == 0:
            @pl.when(t == far)
            def _():
                pp_copy(t, u, side).wait_recv()
                for way in range(WAYS):
                    for copy in rs_copies(t - 1, u, way, False):
                        copy.wait_recv()
                for d in range(WAYS):
                    total = (here(wide.tile(u, d)) + arrived(0, d)) + arrived(1, d)
                    ag[0, packed.tile(u, d), :] = total.astype(jnp.bfloat16)
                if u == last:
                    total = (here(wide.lone()) + arrived_lone(0)) + arrived_lone(1)
                    ag[0, packed.lone(), :] = jnp.concatenate([total, total], axis=0).astype(jnp.bfloat16)
                for way in range(WAYS):
                    ag_copy(0, u, way, False).start()
                ap_copy(0, u, 0).start()
                expand(0, u, range(WAYS), ag, core)
                if u == last:
                    expand_lone(0, ag, core)

    turns = [(u, side) for u in range(UNITS) for side in range(WAYS)]

    @pl.loop(0, far + 1)
    def _(t):
        for i, (u, side) in enumerate(turns):
            if side == 0:
                compute(t, u, side)
            else:
                @pl.when(jnp.logical_and(t > 0, t < far))
                def _():
                    compute(t, u, side)
            if i >= 2:
                ring(t, *turns[i - 2])
            else:
                @pl.when(t > 0)
                def _():
                    ring(t - 1, *turns[i - 2])

    ring(jnp.int32(far), *turns[-2])

    def mates(h, u, way):
        ap_copy(h, u, way).wait_recv()
        expand(slot_of(h, way), u, range(WAYS), ag_pair, 1 - core)
        if u == last:
            expand_lone(slot_of(h, way), ag_pair, 1 - core)

    for h in range(1, far):
        for u in range(UNITS):
            for way in range(WAYS):
                ag_copy(h - 1, u, way, False).wait_recv()
                ag_copy(h, u, way, h == far - 1).start()
                ap_copy(h, u, way).start()
                expand(slot_of(h, way), u, range(WAYS), ag, core)
                if u == last:
                    expand_lone(slot_of(h, way), ag, core)
                if h > 1 or way == 0:
                    mates(h - 1, u, way)
    for u in range(UNITS):
        for way in range(WAYS):
            ag_copy(far - 1, u, way, True).wait_recv()
            ap_copy(far, u, way, True).start()
            expand(far, u, (way,), ag, core)
            mates(far - 1, u, way)
    expand_lone(far, ag, core)
    for u in range(UNITS):
        for way in range(WAYS):
            ap_copy(far, u, way, True).wait_recv()
            expand(far, u, (way,), ag_pair, 1 - core)
    expand_lone(far, ag_pair, 1 - core)

    for u in range(UNITS):
        ap_copy(0, u, 0).wait_send()
        for side in range(WAYS):
            for copy in rs_copies(0, u, side, True):
                copy.wait_send()
            ag_copy(far - 1, u, side, True).wait_send()
            ap_copy(far, u, side, True).wait_send()

    @pl.loop(0, 2 * far)
    def _(q):
        for u in range(UNITS):
            pltpu.make_async_remote_copy(
                src_ref=part.at[1 - core, q, wide.pair(u)], dst_ref=part_in.at[q, wide.pair(u)],
                send_sem=pp_send.at[q, u], recv_sem=pp_recv.at[q, u], device_id={"tp": mate}, device_id_type=MESH).wait_send()

    @pl.loop(1, far)
    def _(t):
        for u in range(UNITS):
            for side in range(WAYS):
                for copy in rs_copies(t, u, side, False):
                    copy.wait_send()
                ag_copy(t - 1, u, side, False).wait_send()
                ap_copy(t, u, side).wait_send()


def solution(mesh):
    chips = mesh.shape["tp"] // CORES

    def local_part(x_loc, w_loc, lengths):
        tokens, depth = x_loc.shape
        columns = w_loc.shape[1]
        n_seq = lengths.shape[0]
        seq_len = tokens // n_seq
        body_rows = (n_seq - 1) * seq_len
        far = chips // 2
        assert columns == chips * UNITS * BLOCK and chips == 2 * far and far >= 3
        wide, packed, low = Rows(body_rows, 8), Rows(body_rows, 16), Rows(body_rows // LOWS, 0)
        dma = pltpu.SemaphoreType.DMA
        held = pltpu.VMEM((chips, packed.total, LANES), jnp.bfloat16)
        vmem = pl.BlockSpec(memory_space=pltpu.VMEM)
        smem = pl.BlockSpec(memory_space=pltpu.SMEM)
        hbm = pl.BlockSpec(memory_space=pl.ANY)
        high = pltpu.VMEM((WAYS, far, packed.total, LANES), jnp.bfloat16)
        lows = pltpu.VMEM((WAYS, far, low.total, LANES), jnp.int16)
        hops = dma((WAYS, far, UNITS))
        return pl.pallas_call(
            functools.partial(reduce_kernel, chips, n_seq, seq_len),
            out_shape=pltpu.VMEM((tokens, columns), jnp.bfloat16),
            in_specs=[smem, hbm, hbm],
            out_specs=vmem,
            scratch_shapes=[
                pltpu.VMEM((tokens, depth), jnp.bfloat16),
                pltpu.VMEM((body_rows + 16, depth), jnp.bfloat16),
                pltpu.VMEM((SLOTS, depth, BLOCK), jnp.bfloat16),
                pltpu.VMEM((CORES, chips, wide.total, LANES), jnp.float32),
                pltpu.VMEM((chips, wide.total, LANES), jnp.float32),
                high, lows, high, lows, held, held,
                pltpu.VMEM((tokens, LANES), jnp.bfloat16),
                pltpu.VMEM((n_seq * 16, LANES), jnp.bfloat16),
                dma,
                dma((SLOTS,)),
                dma((chips, UNITS)), dma((chips, UNITS)),
                hops, hops, hops, hops, hops, hops,
                dma((WAYS, far + 1, UNITS)), dma((WAYS, far + 1, UNITS)),
            ],
            compiler_params=pltpu.CompilerParams(
                collective_id=0, has_side_effects=True, vmem_limit_bytes=54 * 1024 * 1024),
            name="reduce_gather",
        )(lengths, x_loc, w_loc)

    return jax.shard_map(local_part, mesh=mesh, in_specs=(P("data", "tp"), P("tp", None), P("data")), out_specs=P("data", None), check_vma=False)
```

```python
import functools

import jax
import jax.numpy as jnp
from jax import lax
from jax.experimental import pallas as pl
from jax.experimental.pallas import tpu as pltpu
from jax.sharding import PartitionSpec as P

MESH = pl.DeviceIdType.MESH
LANES = 128
CORES = 2
WAYS = 2
UNITS = 3
SLOTS = UNITS * WAYS
AHEAD = 3
BLOCK = CORES * WAYS * LANES
LONE = UNITS * WAYS - 1
LOWS = 3
LEVELS = 39
STEPS = (LEVELS // 2) * 256


def first_single(len_ref, n_seq):
    slot = jnp.int32(n_seq - 1)
    for s in reversed(range(n_seq - 1)):
        slot = jnp.where(len_ref[s] == 1, jnp.int32(s), slot)
    return slot


def split_sum(total, rows):
    high = total.astype(jnp.bfloat16)
    wide = high.astype(jnp.float32)
    left = jnp.round((total - wide) / jnp.where(wide == 0.0, 1.0, wide) * STEPS)
    third = rows // LOWS
    low = (left[:third] * LEVELS + left[third:2 * third]) * LEVELS + left[2 * third:]
    return high, low.astype(jnp.int32).astype(jnp.int16)


def join_sum(high, low):
    code = low.astype(jnp.int32).astype(jnp.float32)
    first = jnp.round(code * (1.0 / LEVELS ** 2))
    rest = code - first * LEVELS ** 2
    second = jnp.round(rest * (1.0 / LEVELS))
    left = jnp.concatenate([first, second, rest - second * LEVELS], axis=0)
    wide = high.astype(jnp.float32)
    return wide + wide * (left * (1.0 / STEPS))


def split_lone(total):
    high = total.astype(jnp.bfloat16).astype(jnp.float32)
    return jnp.concatenate([high, total - high], axis=0).astype(jnp.bfloat16)


def join_lone(both):
    both = both.astype(jnp.float32)
    return both[:8] + both[8:]


class Rows:
    def __init__(self, tall, tail):
        self.tall, self.tail = tall, tail
        self.total = SLOTS * tall + tail

    def lone(self):
        return pl.ds(LONE * self.tall, self.tail)

    def tile(self, u, d):
        i = u * WAYS + d
        return pl.ds(i * self.tall + (self.tail if i >= LONE else 0), self.tall)

    def pair(self, u):
        return pl.ds(u * WAYS * self.tall, WAYS * self.tall + (self.tail if u == UNITS - 1 else 0))

    def half(self, u, d, lone=True):
        i = u * WAYS + d
        more = self.tail if (u == UNITS - 1 and lone) else 0
        start = i * self.tall + (self.tail if (i >= LONE and not lone) else 0)
        return pl.ds(start, self.tall + more)


def reduce_kernel(
    chips, n_seq, seq_len,
    len_ref, x_hbm, w_hbm, y_ref,
    x_raw, xc, wbuf, part, part_in, tx_hi, tx_lo, rx_hi, rx_lo, ag, ag_pair, keep, alone,
    x_sem, w_sem, pp_send, pp_recv, hi_send, hi_recv, lo_send, lo_recv, ag_send, ag_recv, ap_send, ap_recv,
):
    me = lax.axis_index("tp")
    z, core = me // CORES, lax.rem(me, CORES)
    nxt = lax.rem(z + 1, chips) * CORES + core
    prv = lax.rem(z + chips - 1, chips) * CORES + core
    mate = z * CORES + (1 - core)
    body_rows = (n_seq - 1) * seq_len
    far = chips // 2
    last = UNITS - 1
    wide, packed, low = Rows(body_rows, 8), Rows(body_rows, 16), Rows(body_rows // LOWS, 0)

    def place(t, side):
        return jnp.where(t == 0, 0, jnp.where(t == far, 2 * far - 1, 2 * t - 1 + side))

    blocks = chips * UNITS

    def turn(t, u, side):
        middle = UNITS + (t - 1) * SLOTS + u * WAYS + side
        return jnp.where(t == 0, u, jnp.where(t == far, blocks - UNITS + u, middle))

    def w_copy(n):
        ends = jnp.where(n < UNITS, n, n - (blocks - UNITS))
        inner = jnp.logical_and(n >= UNITS, n < blocks - UNITS)
        i = jnp.where(inner, lax.rem(n + (SLOTS - UNITS), SLOTS), ends * WAYS)
        t = jnp.where(n < UNITS, 0, (n + (SLOTS - UNITS)) // SLOTS)
        u, side = i // WAYS, lax.rem(i, WAYS)
        chunk = lax.rem(z + chips + jnp.where(side == 0, t - far, far - t), chips)
        col = pl.multiple_of((chunk * UNITS + u) * BLOCK, BLOCK)
        b = lax.rem(n, SLOTS)
        return pltpu.make_async_copy(w_hbm.at[:, pl.ds(col, BLOCK)], wbuf.at[b], w_sem.at[b])

    x_copy = pltpu.make_async_copy(x_hbm, x_raw, x_sem)
    x_copy.start()
    w_copy(jnp.int32(0)).start()

    barrier = pltpu.get_barrier_semaphore()
    for peer in (mate, nxt, prv):
        pl.semaphore_signal(barrier, inc=1, device_id={"tp": peer}, device_id_type=MESH)

    single = first_single(len_ref, n_seq)
    x_copy.wait()
    w_copy(jnp.int32(1)).start()

    def x_rows(slot, count):
        return x_raw[slot * seq_len:slot * seq_len + count, :]

    for p in range(n_seq - 1):
        xc[p * seq_len:(p + 1) * seq_len, :] = jnp.where(single <= p, x_rows(p + 1, seq_len), x_rows(p, seq_len))
    lone = x_rows(n_seq - 1, 16)
    for s in range(n_seq - 1):
        lone = jnp.where(single == s, x_rows(s, 16), lone)
    xc[body_rows:body_rows + 16, :] = lone
    row = lax.broadcasted_iota(jnp.int32, (seq_len, LANES), 0)
    zero = jnp.bfloat16(0)
    for s in range(n_seq):
        many = jnp.where(single == s, 0, len_ref[s])
        one = jnp.where(single == s, 1, 0)
        keep[s * seq_len:(s + 1) * seq_len, :] = jnp.where(row < many, 1.0, 0.0).astype(jnp.bfloat16)
        alone[s * 16:(s + 1) * 16, :] = jnp.where(row[:16] < one, 1.0, 0.0).astype(jnp.bfloat16)
    pl.semaphore_wait(barrier, 3)

    def out_cols(slot, i, owner):
        chunk = lax.rem(z + chips - slot, chips)
        return pl.ds(pl.multiple_of(((chunk * SLOTS + i) * CORES + owner) * LANES, LANES), LANES)

    def expand(slot, u, ways, ref, owner):
        for d in ways:
            cols = out_cols(slot, u * WAYS + d, owner)
            top = packed.tile(u, d).start
            block = [ref[slot, top + p * seq_len:top + (p + 1) * seq_len, :] for p in range(n_seq - 1)]
            for s in range(n_seq):
                if s == 0 or s == n_seq - 1:
                    rows = block[min(s, n_seq - 2)]
                else:
                    rows = jnp.where(single < s, block[s - 1], block[s])
                mask = keep[s * seq_len:(s + 1) * seq_len, :]
                y_ref[s * seq_len:(s + 1) * seq_len, cols] = jnp.where(mask > zero, rows, zero)

    def expand_lone(slot, ref, owner):
        tail = ref[slot, packed.lone(), :].astype(jnp.float32)
        for i in range(SLOTS):
            cols = out_cols(slot, i, owner)
            value = jnp.broadcast_to(tail[i:i + 1, :], (16, LANES)).astype(jnp.bfloat16)
            for s in range(n_seq):
                rows = slice(s * seq_len, s * seq_len + 16)
                y_ref[rows, cols] = jnp.where(alone[s * 16:(s + 1) * 16, :] > zero, value, y_ref[rows, cols])

    def pp_copy(t, u, side):
        q = place(t, side)
        return pltpu.make_async_remote_copy(
            src_ref=part.at[1 - core, q, wide.pair(u)], dst_ref=part_in.at[q, wide.pair(u)],
            send_sem=pp_send.at[q, u], recv_sem=pp_recv.at[q, u], device_id={"tp": mate}, device_id_type=MESH)

    def rs_copies(t, u, side, far_end):
        peer = prv if side == 0 else nxt
        copies = []
        for tx, rx, ss, rs, rows in ((tx_hi, rx_hi, hi_send, hi_recv, packed), (tx_lo, rx_lo, lo_send, lo_recv, low)):
            where = rows.half(u, side) if far_end else rows.pair(u)
            copies.append(pltpu.make_async_remote_copy(
                src_ref=tx.at[side, t, where], dst_ref=rx.at[side, t, where],
                send_sem=ss.at[side, t, u], recv_sem=rs.at[side, t, u], device_id={"tp": peer}, device_id_type=MESH))
        return copies

    def ag_where(u, way, half):
        return packed.half(u, way, lone=way == 0) if half else packed.pair(u)

    def slot_of(h, way):
        return h if way == 0 else lax.rem(2 * far - h, 2 * far)

    def ag_copy(h, u, way, half):
        where = ag_where(u, way, half)
        return pltpu.make_async_remote_copy(
            src_ref=ag.at[slot_of(h, way), where], dst_ref=ag.at[slot_of(h + 1, way), where],
            send_sem=ag_send.at[way, h, u], recv_sem=ag_recv.at[way, h, u],
            device_id={"tp": nxt if way == 0 else prv}, device_id_type=MESH)

    def ap_copy(h, u, way, half=False):
        where = ag_where(u, way, half)
        return pltpu.make_async_remote_copy(
            src_ref=ag.at[slot_of(h, way), where], dst_ref=ag_pair.at[slot_of(h, way), where],
            send_sem=ap_send.at[way, h, u], recv_sem=ap_recv.at[way, h, u], device_id={"tp": mate}, device_id_type=MESH)

    def compute(t, u, side):
        q = place(t, side)
        n = turn(t, u, side)
        w_copy(n).wait()
        if u == 0 and side == 0:
            @pl.when(t == 0)
            def _():
                for early in range(2, AHEAD):
                    w_copy(jnp.int32(early)).start()

        @pl.when(n + AHEAD < blocks)
        def _():
            w_copy(n + AHEAD).start()

        prod = jnp.dot(xc[...], wbuf[lax.rem(n, SLOTS)], preferred_element_type=jnp.float32)
        for d in range(WAYS):
            i = u * WAYS + d
            for half in range(CORES):
                cols = slice((d * CORES + half) * LANES, (d * CORES + half + 1) * LANES)
                part[half, q, wide.tile(u, d), :] = prod[:body_rows, cols]
                tile = LONE * body_rows
                if i == 0:
                    part[half, q, tile:tile + 8, :] = prod[body_rows:body_rows + 8, cols]
                else:
                    part[half, q, tile + i:tile + i + 1, :] = prod[body_rows:body_rows + 1, cols]
        pp_copy(t, u, side).start()

    def ring(t, u, side):
        q = place(t, side)
        parity = lax.rem(lax.broadcasted_iota(jnp.int32, (8, LANES), 0), WAYS)

        def here(where):
            return part[core, q, where, :] + part_in[q, where, :]

        def arrived(side_, d):
            return join_sum(rx_hi[side_, t - 1, packed.tile(u, d), :], rx_lo[side_, t - 1, low.tile(u, d), :])

        def arrived_lone(side_):
            return join_lone(rx_hi[side_, t - 1, packed.lone(), :])

        def put(side_, d, total):
            tx_hi[side_, t, packed.tile(u, d), :], tx_lo[side_, t, low.tile(u, d), :] = split_sum(total, body_rows)

        def put_lone(side_, total):
            tx_hi[side_, t, packed.lone(), :] = split_lone(total)

        if side == 0:
            @pl.when(t == 0)
            def _():
                pp_copy(t, u, side).wait_recv()
                for d in range(WAYS):
                    put(d, d, here(wide.tile(u, d)))
                    if u == last:
                        put_lone(d, here(wide.lone()))
                    for copy in rs_copies(0, u, d, True):
                        copy.start()

        @pl.when(t == 1)
        def _():
            pp_copy(t, u, side).wait_recv()
            put(side, 1 - side, here(wide.tile(u, 1 - side)))
            for copy in rs_copies(0, u, side, True):
                copy.wait_recv()
            put(side, side, here(wide.tile(u, side)) + arrived(side, side))
            if u == last:
                put_lone(side, here(wide.lone()) + jnp.where(parity == side, arrived_lone(side), 0.0))
            for copy in rs_copies(1, u, side, False):
                copy.start()

        @pl.when(jnp.logical_and(t > 1, t < far))
        def _():
            pp_copy(t, u, side).wait_recv()
            for copy in rs_copies(t - 1, u, side, False):
                copy.wait_recv()
            for d in range(WAYS):
                put(side, d, here(wide.tile(u, d)) + arrived(side, d))
            if u == last:
                put_lone(side, here(wide.lone()) + arrived_lone(side))
            for copy in rs_copies(t, u, side, False):
                copy.start()

        if side == 0:
            @pl.when(t == far)
            def _():
                pp_copy(t, u, side).wait_recv()
                for way in range(WAYS):
                    for copy in rs_copies(t - 1, u, way, False):
                        copy.wait_recv()
                for d in range(WAYS):
                    total = (here(wide.tile(u, d)) + arrived(0, d)) + arrived(1, d)
                    ag[0, packed.tile(u, d), :] = total.astype(jnp.bfloat16)
                if u == last:
                    total = (here(wide.lone()) + arrived_lone(0)) + arrived_lone(1)
                    ag[0, packed.lone(), :] = jnp.concatenate([total, total], axis=0).astype(jnp.bfloat16)
                for way in range(WAYS):
                    ag_copy(0, u, way, False).start()
                ap_copy(0, u, 0).start()
                expand(0, u, range(WAYS), ag, core)
                if u == last:
                    expand_lone(0, ag, core)

    turns = [(u, side) for u in range(UNITS) for side in range(WAYS)]

    @pl.loop(0, far + 1)
    def _(t):
        for i, (u, side) in enumerate(turns):
            if side == 0:
                compute(t, u, side)
            else:
                @pl.when(jnp.logical_and(t > 0, t < far))
                def _():
                    compute(t, u, side)
            if i == 0:
                @pl.when(t == 1)
                def _():
                    ring(jnp.int32(0), UNITS - 1, 0)

                @pl.when(t > 1)
                def _():
                    ring(t - 1, *turns[-1])
            elif side == 1:
                @pl.when(t > 0)
                def _():
                    ring(t, u, 0)
            else:
                @pl.when(t == 0)
                def _():
                    ring(jnp.int32(0), u - 1, 0)

                @pl.when(jnp.logical_and(t > 0, t < far))
                def _():
                    ring(t, u - 1, 1)

    def mates(h, u, way):
        ap_copy(h, u, way).wait_recv()
        expand(slot_of(h, way), u, range(WAYS), ag_pair, 1 - core)
        if u == last:
            expand_lone(slot_of(h, way), ag_pair, 1 - core)

    for h in range(1, far):
        for u in range(UNITS):
            for way in range(WAYS):
                ag_copy(h - 1, u, way, False).wait_recv()
                ag_copy(h, u, way, h == far - 1).start()
                ap_copy(h, u, way).start()
            for way in range(WAYS):
                expand(slot_of(h, way), u, range(WAYS), ag, core)
                if u == last:
                    expand_lone(slot_of(h, way), ag, core)
                if h > 1 or way == 0:
                    mates(h - 1, u, way)
    for u in range(UNITS):
        for way in range(WAYS):
            ag_copy(far - 1, u, way, True).wait_recv()
            ap_copy(far, u, way, True).start()
        for way in range(WAYS):
            expand(far, u, (way,), ag, core)
            mates(far - 1, u, way)
    expand_lone(far, ag, core)
    for u in range(UNITS):
        for way in range(WAYS):
            ap_copy(far, u, way, True).wait_recv()
            expand(far, u, (way,), ag_pair, 1 - core)
    expand_lone(far, ag_pair, 1 - core)

    for u in range(UNITS):
        ap_copy(0, u, 0).wait_send()
        for side in range(WAYS):
            for copy in rs_copies(0, u, side, True):
                copy.wait_send()
            ag_copy(far - 1, u, side, True).wait_send()
            ap_copy(far, u, side, True).wait_send()

    @pl.loop(0, 2 * far)
    def _(q):
        for u in range(UNITS):
            pltpu.make_async_remote_copy(
                src_ref=part.at[1 - core, q, wide.pair(u)], dst_ref=part_in.at[q, wide.pair(u)],
                send_sem=pp_send.at[q, u], recv_sem=pp_recv.at[q, u], device_id={"tp": mate}, device_id_type=MESH).wait_send()

    @pl.loop(1, far)
    def _(t):
        for u in range(UNITS):
            for side in range(WAYS):
                for copy in rs_copies(t, u, side, False):
                    copy.wait_send()
                ag_copy(t - 1, u, side, False).wait_send()
                ap_copy(t, u, side).wait_send()


def solution(mesh):
    chips = mesh.shape["tp"] // CORES

    def local_part(x_loc, w_loc, lengths):
        tokens, depth = x_loc.shape
        columns = w_loc.shape[1]
        n_seq = lengths.shape[0]
        seq_len = tokens // n_seq
        body_rows = (n_seq - 1) * seq_len
        far = chips // 2
        assert columns == chips * UNITS * BLOCK and chips == 2 * far and far >= 3
        wide, packed, low = Rows(body_rows, 8), Rows(body_rows, 16), Rows(body_rows // LOWS, 0)
        dma = pltpu.SemaphoreType.DMA
        held = pltpu.VMEM((chips, packed.total, LANES), jnp.bfloat16)
        vmem = pl.BlockSpec(memory_space=pltpu.VMEM)
        smem = pl.BlockSpec(memory_space=pltpu.SMEM)
        hbm = pl.BlockSpec(memory_space=pl.ANY)
        high = pltpu.VMEM((WAYS, far, packed.total, LANES), jnp.bfloat16)
        lows = pltpu.VMEM((WAYS, far, low.total, LANES), jnp.int16)
        hops = dma((WAYS, far, UNITS))
        return pl.pallas_call(
            functools.partial(reduce_kernel, chips, n_seq, seq_len),
            out_shape=pltpu.VMEM((tokens, columns), jnp.bfloat16),
            in_specs=[smem, hbm, hbm],
            out_specs=vmem,
            scratch_shapes=[
                pltpu.VMEM((tokens, depth), jnp.bfloat16),
                pltpu.VMEM((body_rows + 16, depth), jnp.bfloat16),
                pltpu.VMEM((SLOTS, depth, BLOCK), jnp.bfloat16),
                pltpu.VMEM((CORES, chips, wide.total, LANES), jnp.float32),
                pltpu.VMEM((chips, wide.total, LANES), jnp.float32),
                high, lows, high, lows, held, held,
                pltpu.VMEM((tokens, LANES), jnp.bfloat16),
                pltpu.VMEM((n_seq * 16, LANES), jnp.bfloat16),
                dma,
                dma((SLOTS,)),
                dma((chips, UNITS)), dma((chips, UNITS)),
                hops, hops, hops, hops, hops, hops,
                dma((WAYS, far + 1, UNITS)), dma((WAYS, far + 1, UNITS)),
            ],
            compiler_params=pltpu.CompilerParams(
                collective_id=0, has_side_effects=True, vmem_limit_bytes=54 * 1024 * 1024),
            name="reduce_gather",
        )(lengths, x_loc, w_loc)

    return jax.shard_map(local_part, mesh=mesh, in_specs=(P("data", "tp"), P("tp", None), P("data")), out_specs=P("data", None), check_vma=False)
```

```python
import functools

import jax
import jax.numpy as jnp
from jax import lax
from jax.experimental import pallas as pl
from jax.experimental.pallas import tpu as pltpu
from jax.sharding import PartitionSpec as P

MESH = pl.DeviceIdType.MESH
LANES = 128
CORES = 2
WAYS = 2
UNITS = 3
SLOTS = UNITS * WAYS
AHEAD = 3
BLOCK = CORES * WAYS * LANES
LONE = UNITS * WAYS - 1
LOWS = 3
LEVELS = 39
STEPS = (LEVELS // 2) * 256


def first_single(len_ref, n_seq):
    slot = jnp.int32(n_seq - 1)
    for s in reversed(range(n_seq - 1)):
        slot = jnp.where(len_ref[s] == 1, jnp.int32(s), slot)
    return slot


def split_sum(total, rows):
    high = total.astype(jnp.bfloat16)
    wide = high.astype(jnp.float32)
    left = jnp.round((total - wide) / jnp.where(wide == 0.0, 1.0, wide) * STEPS)
    third = rows // LOWS
    low = (left[:third] * LEVELS + left[third:2 * third]) * LEVELS + left[2 * third:]
    return high, low.astype(jnp.int32).astype(jnp.int16)


def join_sum(high, low):
    code = low.astype(jnp.int32).astype(jnp.float32)
    first = jnp.round(code * (1.0 / LEVELS ** 2))
    rest = code - first * LEVELS ** 2
    second = jnp.round(rest * (1.0 / LEVELS))
    left = jnp.concatenate([first, second, rest - second * LEVELS], axis=0)
    wide = high.astype(jnp.float32)
    return wide + wide * (left * (1.0 / STEPS))


def split_lone(total):
    high = total.astype(jnp.bfloat16).astype(jnp.float32)
    return jnp.concatenate([high, total - high], axis=0).astype(jnp.bfloat16)


def join_lone(both):
    both = both.astype(jnp.float32)
    return both[:8] + both[8:]


class Rows:
    def __init__(self, tall, tail):
        self.tall, self.tail = tall, tail
        self.total = SLOTS * tall + tail

    def lone(self):
        return pl.ds(LONE * self.tall, self.tail)

    def tile(self, u, d):
        i = u * WAYS + d
        return pl.ds(i * self.tall + (self.tail if i >= LONE else 0), self.tall)

    def pair(self, u):
        return pl.ds(u * WAYS * self.tall, WAYS * self.tall + (self.tail if u == UNITS - 1 else 0))

    def half(self, u, d, lone=True):
        i = u * WAYS + d
        more = self.tail if (u == UNITS - 1 and lone) else 0
        start = i * self.tall + (self.tail if (i >= LONE and not lone) else 0)
        return pl.ds(start, self.tall + more)


def reduce_kernel(
    chips, n_seq, seq_len,
    len_ref, x_hbm, w_hbm, y_ref,
    x_raw, xc, wbuf, part, part_in, tx_hi, tx_lo, rx_hi, rx_lo, ag, ag_pair, keep, alone,
    x_sem, w_sem, pp_send, pp_recv, hi_send, hi_recv, lo_send, lo_recv, ag_send, ag_recv, ap_send, ap_recv,
):
    me = lax.axis_index("tp")
    z, core = me // CORES, lax.rem(me, CORES)
    nxt = lax.rem(z + 1, chips) * CORES + core
    prv = lax.rem(z + chips - 1, chips) * CORES + core
    mate = z * CORES + (1 - core)
    body_rows = (n_seq - 1) * seq_len
    far = chips // 2
    last = UNITS - 1
    wide, packed, low = Rows(body_rows, 8), Rows(body_rows, 16), Rows(body_rows // LOWS, 0)

    def place(t, side):
        return jnp.where(t == 0, 0, jnp.where(t == far, 2 * far - 1, 2 * t - 1 + side))

    blocks = chips * UNITS

    def turn(t, u, side):
        middle = UNITS + (t - 1) * SLOTS + u * WAYS + side
        return jnp.where(t == 0, u, jnp.where(t == far, blocks - UNITS + u, middle))

    def w_copy(n):
        ends = jnp.where(n < UNITS, n, n - (blocks - UNITS))
        inner = jnp.logical_and(n >= UNITS, n < blocks - UNITS)
        i = jnp.where(inner, lax.rem(n + (SLOTS - UNITS), SLOTS), ends * WAYS)
        t = jnp.where(n < UNITS, 0, (n + (SLOTS - UNITS)) // SLOTS)
        u, side = i // WAYS, lax.rem(i, WAYS)
        chunk = lax.rem(z + chips + jnp.where(side == 0, t - far, far - t), chips)
        col = pl.multiple_of((chunk * UNITS + u) * BLOCK, BLOCK)
        b = lax.rem(n, SLOTS)
        return pltpu.make_async_copy(w_hbm.at[:, pl.ds(col, BLOCK)], wbuf.at[b], w_sem.at[b])

    x_copy = pltpu.make_async_copy(x_hbm, x_raw, x_sem)
    x_copy.start()
    w_copy(jnp.int32(0)).start()

    barrier = pltpu.get_barrier_semaphore()
    for peer in (mate, nxt, prv):
        pl.semaphore_signal(barrier, inc=1, device_id={"tp": peer}, device_id_type=MESH)

    single = first_single(len_ref, n_seq)
    x_copy.wait()
    w_copy(jnp.int32(1)).start()

    def x_rows(slot, count):
        return x_raw[slot * seq_len:slot * seq_len + count, :]

    for p in range(n_seq - 1):
        xc[p * seq_len:(p + 1) * seq_len, :] = jnp.where(single <= p, x_rows(p + 1, seq_len), x_rows(p, seq_len))
    lone = x_rows(n_seq - 1, 16)
    for s in range(n_seq - 1):
        lone = jnp.where(single == s, x_rows(s, 16), lone)
    xc[body_rows:body_rows + 16, :] = lone
    row = lax.broadcasted_iota(jnp.int32, (seq_len, LANES), 0)
    zero = jnp.bfloat16(0)
    for s in range(n_seq):
        many = jnp.where(single == s, 0, len_ref[s])
        one = jnp.where(single == s, 1, 0)
        keep[s * seq_len:(s + 1) * seq_len, :] = jnp.where(row < many, 1.0, 0.0).astype(jnp.bfloat16)
        alone[s * 16:(s + 1) * 16, :] = jnp.where(row[:16] < one, 1.0, 0.0).astype(jnp.bfloat16)
    pl.semaphore_wait(barrier, 3)

    def out_cols(slot, i, owner):
        chunk = lax.rem(z + chips - slot, chips)
        return pl.ds(pl.multiple_of(((chunk * SLOTS + i) * CORES + owner) * LANES, LANES), LANES)

    def expand(slot, u, ways, ref, owner):
        for d in ways:
            cols = out_cols(slot, u * WAYS + d, owner)
            top = packed.tile(u, d).start
            block = [ref[slot, top + p * seq_len:top + (p + 1) * seq_len, :] for p in range(n_seq - 1)]
            for s in range(n_seq):
                if s == 0 or s == n_seq - 1:
                    rows = block[min(s, n_seq - 2)]
                else:
                    rows = jnp.where(single < s, block[s - 1], block[s])
                mask = keep[s * seq_len:(s + 1) * seq_len, :]
                y_ref[s * seq_len:(s + 1) * seq_len, cols] = jnp.where(mask > zero, rows, zero)

    def expand_lone(slot, ref, owner):
        tail = ref[slot, packed.lone(), :].astype(jnp.float32)
        for i in range(SLOTS):
            cols = out_cols(slot, i, owner)
            value = jnp.broadcast_to(tail[i:i + 1, :], (16, LANES)).astype(jnp.bfloat16)
            for s in range(n_seq):
                rows = slice(s * seq_len, s * seq_len + 16)
                y_ref[rows, cols] = jnp.where(alone[s * 16:(s + 1) * 16, :] > zero, value, y_ref[rows, cols])

    def pp_copy(t, u, side):
        q = place(t, side)
        return pltpu.make_async_remote_copy(
            src_ref=part.at[1 - core, q, wide.pair(u)], dst_ref=part_in.at[q, wide.pair(u)],
            send_sem=pp_send.at[q, u], recv_sem=pp_recv.at[q, u], device_id={"tp": mate}, device_id_type=MESH)

    def rs_copies(t, u, side, far_end):
        peer = prv if side == 0 else nxt
        copies = []
        for tx, rx, ss, rs, rows in ((tx_hi, rx_hi, hi_send, hi_recv, packed), (tx_lo, rx_lo, lo_send, lo_recv, low)):
            where = rows.half(u, side) if far_end else rows.pair(u)
            copies.append(pltpu.make_async_remote_copy(
                src_ref=tx.at[side, t, where], dst_ref=rx.at[side, t, where],
                send_sem=ss.at[side, t, u], recv_sem=rs.at[side, t, u], device_id={"tp": peer}, device_id_type=MESH))
        return copies

    def ag_where(u, way, half):
        return packed.half(u, way, lone=way == 0) if half else packed.pair(u)

    def slot_of(h, way):
        return h if way == 0 else lax.rem(2 * far - h, 2 * far)

    def ag_copy(h, u, way, half):
        where = ag_where(u, way, half)
        return pltpu.make_async_remote_copy(
            src_ref=ag.at[slot_of(h, way), where], dst_ref=ag.at[slot_of(h + 1, way), where],
            send_sem=ag_send.at[way, h, u], recv_sem=ag_recv.at[way, h, u],
            device_id={"tp": nxt if way == 0 else prv}, device_id_type=MESH)

    def ap_copy(h, u, way, half=False):
        where = ag_where(u, way, half)
        return pltpu.make_async_remote_copy(
            src_ref=ag.at[slot_of(h, way), where], dst_ref=ag_pair.at[slot_of(h, way), where],
            send_sem=ap_send.at[way, h, u], recv_sem=ap_recv.at[way, h, u], device_id={"tp": mate}, device_id_type=MESH)

    def compute(t, u, side):
        q = place(t, side)
        n = turn(t, u, side)
        w_copy(n).wait()
        if u == 0 and side == 0:
            @pl.when(t == 0)
            def _():
                for early in range(2, AHEAD):
                    w_copy(jnp.int32(early)).start()

        @pl.when(n + AHEAD < blocks)
        def _():
            w_copy(n + AHEAD).start()

        prod = jnp.dot(xc[...], wbuf[lax.rem(n, SLOTS)], preferred_element_type=jnp.float32)
        for d in range(WAYS):
            i = u * WAYS + d
            for half in range(CORES):
                cols = slice((d * CORES + half) * LANES, (d * CORES + half + 1) * LANES)
                part[half, q, wide.tile(u, d), :] = prod[:body_rows, cols]
                tile = LONE * body_rows
                if i == 0:
                    part[half, q, tile:tile + 8, :] = prod[body_rows:body_rows + 8, cols]
                else:
                    part[half, q, tile + i:tile + i + 1, :] = prod[body_rows:body_rows + 1, cols]
        pp_copy(t, u, side).start()

    def ring(t, u, side):
        q = place(t, side)
        parity = lax.rem(lax.broadcasted_iota(jnp.int32, (8, LANES), 0), WAYS)

        def here(where):
            return part[core, q, where, :] + part_in[q, where, :]

        def arrived(side_, d):
            return join_sum(rx_hi[side_, t - 1, packed.tile(u, d), :], rx_lo[side_, t - 1, low.tile(u, d), :])

        def arrived_lone(side_):
            return join_lone(rx_hi[side_, t - 1, packed.lone(), :])

        def put(side_, d, total):
            tx_hi[side_, t, packed.tile(u, d), :], tx_lo[side_, t, low.tile(u, d), :] = split_sum(total, body_rows)

        def put_lone(side_, total):
            tx_hi[side_, t, packed.lone(), :] = split_lone(total)

        if side == 0:
            @pl.when(t == 0)
            def _():
                pp_copy(t, u, side).wait_recv()
                for d in range(WAYS):
                    put(d, d, here(wide.tile(u, d)))
                    if u == last:
                        put_lone(d, here(wide.lone()))
                    for copy in rs_copies(0, u, d, True):
                        copy.start()

        @pl.when(t == 1)
        def _():
            pp_copy(t, u, side).wait_recv()
            put(side, 1 - side, here(wide.tile(u, 1 - side)))
            for copy in rs_copies(0, u, side, True):
                copy.wait_recv()
            put(side, side, here(wide.tile(u, side)) + arrived(side, side))
            if u == last:
                put_lone(side, here(wide.lone()) + jnp.where(parity == side, arrived_lone(side), 0.0))
            for copy in rs_copies(1, u, side, False):
                copy.start()

        @pl.when(jnp.logical_and(t > 1, t < far))
        def _():
            pp_copy(t, u, side).wait_recv()
            for copy in rs_copies(t - 1, u, side, False):
                copy.wait_recv()
            for d in range(WAYS):
                put(side, d, here(wide.tile(u, d)) + arrived(side, d))
            if u == last:
                put_lone(side, here(wide.lone()) + arrived_lone(side))
            for copy in rs_copies(t, u, side, False):
                copy.start()

        if side == 0:
            @pl.when(t == far)
            def _():
                pp_copy(t, u, side).wait_recv()
                for way in range(WAYS):
                    for copy in rs_copies(t - 1, u, way, False):
                        copy.wait_recv()
                for d in range(WAYS):
                    total = (here(wide.tile(u, d)) + arrived(0, d)) + arrived(1, d)
                    ag[0, packed.tile(u, d), :] = total.astype(jnp.bfloat16)
                if u == last:
                    total = (here(wide.lone()) + arrived_lone(0)) + arrived_lone(1)
                    ag[0, packed.lone(), :] = jnp.concatenate([total, total], axis=0).astype(jnp.bfloat16)
                for way in range(WAYS):
                    ag_copy(0, u, way, False).start()
                ap_copy(0, u, 0).start()

    turns = [(u, side) for u in range(UNITS) for side in range(WAYS)]

    @pl.loop(0, far + 1)
    def _(t):
        for i, (u, side) in enumerate(turns):
            if side == 0:
                compute(t, u, side)
            else:
                @pl.when(jnp.logical_and(t > 0, t < far))
                def _():
                    compute(t, u, side)
            if i == 0:
                @pl.when(t == 1)
                def _():
                    ring(jnp.int32(0), UNITS - 1, 0)

                @pl.when(t > 1)
                def _():
                    ring(t - 1, *turns[-1])
            elif side == 1:
                @pl.when(t > 0)
                def _():
                    ring(t, u, 0)
            else:
                @pl.when(t == 0)
                def _():
                    ring(jnp.int32(0), u - 1, 0)

                @pl.when(jnp.logical_and(t > 0, t < far))
                def _():
                    ring(t, u - 1, 1)

    def mates(h, u, way):
        ap_copy(h, u, way).wait_recv()
        expand(slot_of(h, way), u, range(WAYS), ag_pair, 1 - core)
        if u == last:
            expand_lone(slot_of(h, way), ag_pair, 1 - core)

    for u in range(UNITS):
        expand(0, u, range(WAYS), ag, core)
    expand_lone(0, ag, core)
    for h in range(1, far):
        for u in range(UNITS):
            for way in range(WAYS):
                ag_copy(h - 1, u, way, False).wait_recv()
                ag_copy(h, u, way, h == far - 1).start()
                ap_copy(h, u, way).start()
            for way in range(WAYS):
                expand(slot_of(h, way), u, range(WAYS), ag, core)
                if u == last:
                    expand_lone(slot_of(h, way), ag, core)
                if h > 1 or way == 0:
                    mates(h - 1, u, way)
    for u in range(UNITS):
        for way in range(WAYS):
            ag_copy(far - 1, u, way, True).wait_recv()
            ap_copy(far, u, way, True).start()
        for way in range(WAYS):
            expand(far, u, (way,), ag, core)
            mates(far - 1, u, way)
    expand_lone(far, ag, core)
    for u in range(UNITS):
        for way in range(WAYS):
            ap_copy(far, u, way, True).wait_recv()
            expand(far, u, (way,), ag_pair, 1 - core)
    expand_lone(far, ag_pair, 1 - core)

    for u in range(UNITS):
        ap_copy(0, u, 0).wait_send()
        for side in range(WAYS):
            for copy in rs_copies(0, u, side, True):
                copy.wait_send()
            ag_copy(far - 1, u, side, True).wait_send()
            ap_copy(far, u, side, True).wait_send()

    @pl.loop(0, 2 * far)
    def _(q):
        for u in range(UNITS):
            pltpu.make_async_remote_copy(
                src_ref=part.at[1 - core, q, wide.pair(u)], dst_ref=part_in.at[q, wide.pair(u)],
                send_sem=pp_send.at[q, u], recv_sem=pp_recv.at[q, u], device_id={"tp": mate}, device_id_type=MESH).wait_send()

    @pl.loop(1, far)
    def _(t):
        for u in range(UNITS):
            for side in range(WAYS):
                for copy in rs_copies(t, u, side, False):
                    copy.wait_send()
                ag_copy(t - 1, u, side, False).wait_send()
                ap_copy(t, u, side).wait_send()


def solution(mesh):
    chips = mesh.shape["tp"] // CORES

    def local_part(x_loc, w_loc, lengths):
        tokens, depth = x_loc.shape
        columns = w_loc.shape[1]
        n_seq = lengths.shape[0]
        seq_len = tokens // n_seq
        body_rows = (n_seq - 1) * seq_len
        far = chips // 2
        assert columns == chips * UNITS * BLOCK and chips == 2 * far and far >= 3
        wide, packed, low = Rows(body_rows, 8), Rows(body_rows, 16), Rows(body_rows // LOWS, 0)
        dma = pltpu.SemaphoreType.DMA
        held = pltpu.VMEM((chips, packed.total, LANES), jnp.bfloat16)
        vmem = pl.BlockSpec(memory_space=pltpu.VMEM)
        smem = pl.BlockSpec(memory_space=pltpu.SMEM)
        hbm = pl.BlockSpec(memory_space=pl.ANY)
        high = pltpu.VMEM((WAYS, far, packed.total, LANES), jnp.bfloat16)
        lows = pltpu.VMEM((WAYS, far, low.total, LANES), jnp.int16)
        hops = dma((WAYS, far, UNITS))
        return pl.pallas_call(
            functools.partial(reduce_kernel, chips, n_seq, seq_len),
            out_shape=pltpu.VMEM((tokens, columns), jnp.bfloat16),
            in_specs=[smem, hbm, hbm],
            out_specs=vmem,
            scratch_shapes=[
                pltpu.VMEM((tokens, depth), jnp.bfloat16),
                pltpu.VMEM((body_rows + 16, depth), jnp.bfloat16),
                pltpu.VMEM((SLOTS, depth, BLOCK), jnp.bfloat16),
                pltpu.VMEM((CORES, chips, wide.total, LANES), jnp.float32),
                pltpu.VMEM((chips, wide.total, LANES), jnp.float32),
                high, lows, high, lows, held, held,
                pltpu.VMEM((tokens, LANES), jnp.bfloat16),
                pltpu.VMEM((n_seq * 16, LANES), jnp.bfloat16),
                dma,
                dma((SLOTS,)),
                dma((chips, UNITS)), dma((chips, UNITS)),
                hops, hops, hops, hops, hops, hops,
                dma((WAYS, far + 1, UNITS)), dma((WAYS, far + 1, UNITS)),
            ],
            compiler_params=pltpu.CompilerParams(
                collective_id=0, has_side_effects=True, vmem_limit_bytes=54 * 1024 * 1024),
            name="reduce_gather",
        )(lengths, x_loc, w_loc)

    return jax.shard_map(local_part, mesh=mesh, in_specs=(P("data", "tp"), P("tp", None), P("data")), out_specs=P("data", None), check_vma=False)
```
